512 devices in a mesh: owner: 64 (over y, x, core), rows: 8 (over z).
Axes of the slice: x: 4, y: 8, z: 8, core: 2. Of those that a mesh axis runs over, the one named last changes fastest.
Arguments:
- train_down: float32 [64, 1024, 2048], P('owner', None, 'rows'), may hold values from -0.1875 to 0.1875
- router_weight: float32 [2048, 64], P('rows', 'owner'), may hold values from -0.125 to 0.125
- router_gain: float32 [2048], P('rows'), may hold values from 0.25 to 1.75
Outputs:
- ready_down: bfloat16 [64, 2048, 1024], P('owner')
- serve_router: bfloat16 [2048, 64], replicated
The draws below stay inside these ranges and needn't reach their ends.
All inputs are finite; a program needn't handle non-finite values.
Results may differ from the reference program's by a relative error of at most 0.001.
Values may be sent and summed in bfloat16 or wider, within the bound.
A program may use at most 64 MiB of HBM per device.

```python
import jax
import jax.numpy as jnp

EXPERTS = 64
D_MODEL = 2048
D_EXPERT = 1024


def block_levels(key, extent, shards, least, top_value):
    factor_of = 1.0
    for dim, blocks in shards:
        steps = jax.random.uniform(jax.random.fold_in(jax.random.fold_in(key, 6), dim), (blocks,), jnp.float32, least / len(shards), top_value / len(shards))
        factor_of = factor_of * jnp.repeat(jnp.exp(steps), extent[dim] // blocks).reshape((-1,) + (1,) * (len(extent) - 1 - dim))
    return factor_of


def noise(stream_key, shape, spread, most, split=(), dtype=jnp.bfloat16):
    factor_of = block_levels(stream_key, shape, split, -0.22, 0.18) if split else 1.0
    values = jax.random.normal(stream_key, shape, jnp.float32) * spread * factor_of
    return jnp.minimum(jnp.maximum(values, -most), most).astype(dtype)


def setup_inputs(seed: int = 0) -> dict:
    streams_of = jax.random.split(jax.random.key(seed), 4)
    return {
        "train_down": noise(streams_of[0], (EXPERTS, D_EXPERT, D_MODEL), D_EXPERT ** -0.5, 0.1875, ((0, 64), (2, 8)), jnp.float32),
        "router_weight": noise(streams_of[1], (D_MODEL, EXPERTS), D_MODEL ** -0.5, 0.125, ((0, 8), (1, 64)), jnp.float32),
        "router_gain": jnp.clip(1.0 + 0.15 * jax.random.normal(streams_of[2], (D_MODEL,), jnp.float32), 0.25, 1.75),
    }


def reference(train_down, router_weight, router_gain):
    ready_down = train_down.astype(jnp.bfloat16)
    ready_down = jnp.transpose(ready_down, (0, 2, 1))
    serve_router = (router_weight * router_gain[:, None]).astype(jnp.bfloat16)
    return ready_down, serve_router
```

```python
import functools

import jax
import jax.numpy as jnp
from jax import lax
from jax.experimental import pallas as pl
from jax.experimental.pallas import tpu as pltpu
from jax.sharding import PartitionSpec as P

MESH = pl.DeviceIdType.MESH
NY, NX, NC, NZ = 8, 4, 2, 8
EXPERT = 1024
CUT = 256
LANES = 128
CHUNKS = EXPERT // LANES
HALF = CHUNKS // 2
FULL_STEPS = NZ // 2 - 1
EVENTS = FULL_STEPS * CHUNKS + HALF


def gather_kernel(
    down_ref, weight_ref, gain_ref,
    blocks_ref, router_ref,
    down, weight, gain, columns,
    in_sem, small_sem,
    send_up, recv_up, send_dn, recv_dn,
    send_z, recv_z, send_y, recv_y, send_x, recv_x, send_c, recv_c,
):
    owner = lax.axis_index("owner")
    z = lax.axis_index("rows")
    c = lax.rem(owner, NC)
    x = lax.rem(owner // NC, NX)
    y = owner // (NC * NX)

    def device(yy, xx, cc, zz):
        return {"owner": (yy * NX + xx) * NC + cc, "rows": zz}

    def z_peer(d):
        return device(y, x, c, lax.rem(z + d, NZ))

    def y_peer(d):
        return device(lax.rem(y + d, NY), x, c, z)

    def x_peer(d):
        return device(y, lax.rem(x + d, NX), c, z)

    def c_peer():
        return device(y, x, NC - 1 - c, z)

    loads = []
    for k in range(CHUNKS):
        part = pl.ds(k * LANES, LANES)
        loads.append(pltpu.make_async_copy(down_ref.at[part], down.at[part], in_sem.at[k]))
    load_weight = pltpu.make_async_copy(weight_ref, weight, small_sem.at[0])
    load_gain = pltpu.make_async_copy(gain_ref, gain, small_sem.at[1])
    loads[0].start()
    load_weight.start()
    load_gain.start()
    for k in range(1, CHUNKS):
        loads[k].start()

    barrier = pltpu.get_barrier_semaphore()
    peers = [z_peer(d) for d in range(1, NZ)] + [y_peer(d) for d in range(1, NY)]
    peers += [x_peer(d) for d in range(1, NX)] + [c_peer()]
    for peer in peers:
        pl.semaphore_signal(barrier, inc=1, device_id=peer, device_id_type=MESH)

    def turn(k):
        loads[k].wait()
        piece = down[k * LANES : (k + 1) * LANES, :]
        blocks_ref[z, k] = jnp.transpose(piece).astype(jnp.bfloat16)

    def remote(ref, send, recv, peer):
        return pltpu.make_async_remote_copy(
            src_ref=ref, dst_ref=ref, send_sem=send, recv_sem=recv,
            device_id=peer, device_id_type=MESH,
        )

    def chunk_up(step, k):
        slot = blocks_ref.at[lax.rem(z + NZ - step, NZ), k]
        i = step * CHUNKS + k
        return remote(slot, send_up.at[i], recv_up.at[i], z_peer(1))

    def chunk_dn(step, k):
        slot = blocks_ref.at[lax.rem(z + step, NZ), k]
        i = step * CHUNKS + (k if step < FULL_STEPS else k - HALF)
        return remote(slot, send_dn.at[i], recv_dn.at[i], z_peer(NZ - 1))

    def arrive_up(step, k):
        slot = blocks_ref.at[lax.rem(z + NZ - step - 1, NZ), k]
        i = step * CHUNKS + k
        remote(slot, send_up.at[i], recv_up.at[i], z_peer(1)).wait_recv()

    def arrive_dn(step, k):
        slot = blocks_ref.at[lax.rem(z + step + 1, NZ), k]
        i = step * CHUNKS + (k if step < FULL_STEPS else k - HALF)
        remote(slot, send_dn.at[i], recv_dn.at[i], z_peer(NZ - 1)).wait_recv()

    sent = []

    def send(copy):
        copy.start()
        sent.append(copy)

    turn(0)
    load_weight.wait()
    load_gain.wait()
    columns[y, x, c, z] = weight[...] * gain[...]
    turn(1)
    pl.semaphore_wait(barrier, len(peers))

    for d in range(1, NZ):
        send(remote(columns.at[y, x, c, z], send_z.at[d - 1], recv_z.at[d - 1], z_peer(d)))
    for k in range(CHUNKS):
        if k >= 1 and k + 1 < CHUNKS:
            turn(k + 1)
        send(chunk_up(0, k))
        send(chunk_dn(0, k))

    def router_y():
        for d in range(1, NZ):
            slot = columns.at[y, x, c, lax.rem(z + NZ - d, NZ)]
            remote(slot, send_z.at[d - 1], recv_z.at[d - 1], z_peer(d)).wait_recv()
        for d in range(1, NY):
            send(remote(columns.at[y, x, c], send_y.at[d - 1], recv_y.at[d - 1], y_peer(d)))

    def router_x():
        for d in range(1, NY):
            slot = columns.at[lax.rem(y + NY - d, NY), x, c]
            remote(slot, send_y.at[d - 1], recv_y.at[d - 1], y_peer(d)).wait_recv()
        for d in range(1, NX):
            send(remote(columns.at[:, x, c], send_x.at[d - 1], recv_x.at[d - 1], x_peer(d)))

    def router_c():
        for d in range(1, NX):
            slot = columns.at[:, lax.rem(x + NX - d, NX), c]
            remote(slot, send_x.at[d - 1], recv_x.at[d - 1], x_peer(d)).wait_recv()
        send(remote(columns.at[:, :, c], send_c, recv_c, c_peer()))

    def router_out():
        slot = columns.at[:, :, NC - 1 - c]
        remote(slot, send_c, recv_c, c_peer()).wait_recv()
        for j in range(NZ * 2):
            part = columns[:, :, :, j // 2, j % 2, :].reshape(NY * NX * NC, LANES)
            router_ref[:, j * LANES : (j + 1) * LANES] = part.astype(jnp.bfloat16)

    extras = {(0, 6): router_y, (1, 1): router_x, (1, 5): router_c, (2, 2): router_out}
    for step in range(FULL_STEPS):
        last = step + 1 == FULL_STEPS
        for k in range(CHUNKS):
            arrive_up(step, k)
            if not last or k < HALF:
                send(chunk_up(step + 1, k))
            arrive_dn(step, k)
            if not last or k >= HALF:
                send(chunk_dn(step + 1, k))
            if (step, k) in extras:
                extras[step, k]()
    for k in range(HALF):
        arrive_up(FULL_STEPS, k)
        arrive_dn(FULL_STEPS, k + HALF)
    for copy in sent:
        copy.wait_send()


def place_kernel(blocks_ref, router_ref, down_out, router_out, sem, router_sem):
    copies = []
    for b in range(NZ):
        for k in range(CHUNKS):
            dst = down_out.at[pl.ds(b * CUT, CUT), pl.ds(k * LANES, LANES)]
            copies.append(pltpu.make_async_copy(blocks_ref.at[b, k], dst, sem.at[b, k]))
    copies.append(pltpu.make_async_copy(router_ref, router_out, router_sem))
    for copy in copies:
        copy.start()
    for copy in copies:
        copy.wait()


def on_device(train_down, router_weight, router_gain):
    anywhere = pl.BlockSpec(memory_space=pltpu.HBM)
    vmem = pl.BlockSpec(memory_space=pltpu.VMEM)
    owners = NY * NX * NC
    dma = pltpu.SemaphoreType.DMA
    blocks, router = pl.pallas_call(
        gather_kernel,
        name="gather",
        out_shape=(
            jax.ShapeDtypeStruct((NZ, CHUNKS, CUT, LANES), jnp.bfloat16),
            jax.ShapeDtypeStruct((owners, NZ * CUT), jnp.bfloat16),
        ),
        in_specs=[anywhere] * 3,
        out_specs=(vmem, vmem),
        scratch_shapes=[
            pltpu.VMEM((EXPERT, CUT), jnp.float32),
            pltpu.VMEM((2, LANES), jnp.float32),
            pltpu.VMEM((2, LANES), jnp.float32),
            pltpu.VMEM((NY, NX, NC, NZ, 2, LANES), jnp.float32),
            dma((CHUNKS,)),
            dma((2,)),
            dma((EVENTS,)), dma((EVENTS,)), dma((EVENTS,)), dma((EVENTS,)),
            dma((NZ - 1,)), dma((NZ - 1,)),
            dma((NY - 1,)), dma((NY - 1,)),
            dma((NX - 1,)), dma((NX - 1,)),
            dma, dma,
        ],
        compiler_params=pltpu.CompilerParams(
            collective_id=0, has_side_effects=True, vmem_limit_bytes=16 << 20
        ),
    )(
        *(pltpu.with_memory_space_constraint(array, pltpu.HBM) for array in (
            train_down.reshape(EXPERT, CUT),
            router_weight.reshape(2, LANES),
            router_gain.reshape(2, LANES),
        )),
    )
    ready, serve = pl.pallas_call(
        place_kernel,
        name="place",
        out_shape=(
            jax.ShapeDtypeStruct((NZ * CUT, EXPERT), jnp.bfloat16),
            jax.ShapeDtypeStruct((owners, NZ * CUT), jnp.bfloat16),
        ),
        in_specs=[vmem, vmem],
        out_specs=(anywhere, anywhere),
        scratch_shapes=[dma((NZ, CHUNKS)), dma],
        compiler_params=pltpu.CompilerParams(vmem_limit_bytes=16 << 20),
    )(blocks, router)
    return ready[None], serve.T


def solution(mesh):
    in_specs = (P("owner", None, "rows"), P("rows", "owner"), P("rows"))
    out_specs = (P("owner", None, None), P())
    return jax.shard_map(
        on_device, mesh=mesh, in_specs=in_specs, out_specs=out_specs, check_vma=False
    )
```

```python
import functools

import jax
import jax.numpy as jnp
from jax import lax
from jax.experimental import pallas as pl
from jax.experimental.pallas import tpu as pltpu
from jax.sharding import PartitionSpec as P

MESH = pl.DeviceIdType.MESH
NY, NX, NC, NZ = 8, 4, 2, 8
EXPERT = 1024
CUT = 256
LANES = 128
CHUNKS = EXPERT // LANES
FULL_STEPS = NZ // 2 - 1
EVENTS = (FULL_STEPS + 1) * CHUNKS
ROUNDS = 3
SHARE = (2, 3, 4, 4, 4, 4, 4, 4)


def share_of(z):
    share = jnp.int32(SHARE[NZ - 1])
    for place in range(NZ - 1):
        share = jnp.where(z == place, jnp.int32(SHARE[place]), share)
    return share


def gather_kernel(
    down_ref, weight_ref, gain_ref,
    blocks_ref, router_ref,
    down, weight, gain, columns,
    in_sem, small_sem,
    round_sem,
    send_up, recv_up, send_dn, recv_dn,
    send_z, recv_z, send_y, recv_y, send_x, recv_x, send_c, recv_c,
):
    owner = lax.axis_index("owner")
    z = lax.axis_index("rows")
    c = lax.rem(owner, NC)
    x = lax.rem(owner // NC, NX)
    y = owner // (NC * NX)

    def device(yy, xx, cc, zz):
        return {"owner": (yy * NX + xx) * NC + cc, "rows": zz}

    def z_peer(d):
        return device(y, x, c, lax.rem(z + d, NZ))

    def y_peer(d):
        return device(lax.rem(y + d, NY), x, c, z)

    def x_peer(d):
        return device(y, lax.rem(x + d, NX), c, z)

    def c_peer():
        return device(y, x, NC - 1 - c, z)

    loads = []
    for k in range(CHUNKS):
        part = pl.ds(k * LANES, LANES)
        loads.append(pltpu.make_async_copy(down_ref.at[part], down.at[part], in_sem.at[k]))
    load_weight = pltpu.make_async_copy(weight_ref, weight, small_sem.at[0])
    load_gain = pltpu.make_async_copy(gain_ref, gain, small_sem.at[1])
    loads[0].start()
    load_weight.start()
    load_gain.start()
    for k in range(1, CHUNKS):
        loads[k].start()

    barrier = pltpu.get_barrier_semaphore()
    near = [z_peer(1), z_peer(NZ - 1), y_peer(1), y_peer(NY - 1), x_peer(1), x_peer(NX - 1)]

    def greet(sem, peers):
        for peer in peers:
            pl.semaphore_signal(sem, inc=1, device_id=peer, device_id_type=MESH)

    greet(barrier, [*near, c_peer()])
    share = share_of(z)
    share_above = share_of(lax.rem(z + 1, NZ))
    share_below = share_of(lax.rem(z + NZ - 1, NZ))

    def turn(k):
        loads[k].wait()
        piece = down[k * LANES : (k + 1) * LANES, :]
        blocks_ref[z, k] = jnp.transpose(piece).astype(jnp.bfloat16)

    def remote(ref, send, recv, peer):
        return pltpu.make_async_remote_copy(
            src_ref=ref, dst_ref=ref, send_sem=send, recv_sem=recv,
            device_id=peer, device_id_type=MESH,
        )

    def chunk_up(step, k):
        slot = blocks_ref.at[lax.rem(z + NZ - step, NZ), k]
        i = step * CHUNKS + k
        return remote(slot, send_up.at[i], recv_up.at[i], z_peer(1))

    def chunk_dn(step, k):
        slot = blocks_ref.at[lax.rem(z + step, NZ), k]
        i = step * CHUNKS + k
        return remote(slot, send_dn.at[i], recv_dn.at[i], z_peer(NZ - 1))

    def arrive_up(step, k):
        slot = blocks_ref.at[lax.rem(z + NZ - step - 1, NZ), k]
        i = step * CHUNKS + k
        remote(slot, send_up.at[i], recv_up.at[i], z_peer(1)).wait_recv()

    def arrive_dn(step, k):
        slot = blocks_ref.at[lax.rem(z + step + 1, NZ), k]
        i = step * CHUNKS + k
        remote(slot, send_dn.at[i], recv_dn.at[i], z_peer(NZ - 1)).wait_recv()

    sent = []

    def send(copy, when=None):
        if when is None:
            copy.start()
        else:
            pl.when(when)(copy.start)
        sent.append((copy, when))

    turn(0)
    load_weight.wait()
    load_gain.wait()
    columns[y, x, c, z] = weight[...] * gain[...]
    turn(1)
    pl.semaphore_wait(barrier, len(near) + 1)

    for k in range(CHUNKS):
        if k >= 1 and k + 1 < CHUNKS:
            turn(k + 1)
        send(chunk_up(0, k))
        send(chunk_dn(0, k))
        if k == 0:
            greet(round_sem.at[0], near)
    for r in range(ROUNDS):
        pl.semaphore_wait(round_sem.at[r], len(near))
        if r + 1 < ROUNDS:
            greet(round_sem.at[r + 1], near)
    for d in range(1, NZ):
        send(remote(columns.at[y, x, c, z], send_z.at[d - 1], recv_z.at[d - 1], z_peer(d)))

    def router_y():
        for d in range(1, NZ):
            slot = columns.at[y, x, c, lax.rem(z + NZ - d, NZ)]
            remote(slot, send_z.at[d - 1], recv_z.at[d - 1], z_peer(d)).wait_recv()
        for d in range(1, NY):
            send(remote(columns.at[y, x, c], send_y.at[d - 1], recv_y.at[d - 1], y_peer(d)))

    def router_x():
        for d in range(1, NY):
            slot = columns.at[lax.rem(y + NY - d, NY), x, c]
            remote(slot, send_y.at[d - 1], recv_y.at[d - 1], y_peer(d)).wait_recv()
        for d in range(1, NX):
            send(remote(columns.at[:, x, c], send_x.at[d - 1], recv_x.at[d - 1], x_peer(d)))

    def router_c():
        for d in range(1, NX):
            slot = columns.at[:, lax.rem(x + NX - d, NX), c]
            remote(slot, send_x.at[d - 1], recv_x.at[d - 1], x_peer(d)).wait_recv()
        send(remote(columns.at[:, :, c], send_c, recv_c, c_peer()))

    def router_out():
        slot = columns.at[:, :, NC - 1 - c]
        remote(slot, send_c, recv_c, c_peer()).wait_recv()
        for j in range(NZ * 2):
            part = columns[:, :, :, j // 2, j % 2, :].reshape(NY * NX * NC, LANES)
            router_ref[:, j * LANES : (j + 1) * LANES] = part.astype(jnp.bfloat16)

    extras = {9: router_y, 14: router_x, 17: router_c, 20: router_out}
    for step in range(FULL_STEPS):
        last = step + 1 == FULL_STEPS
        for k in range(CHUNKS):
            arrive_up(step, k)
            send(chunk_up(step + 1, k), k < share_above if last else None)
            arrive_dn(step, k)
            send(chunk_dn(step + 1, k), k >= share_below if last else None)
            if step * CHUNKS + k in extras:
                extras[step * CHUNKS + k]()
    for k in range(CHUNKS):
        pl.when(k < share)(functools.partial(arrive_up, FULL_STEPS, k))
        pl.when(k >= share)(functools.partial(arrive_dn, FULL_STEPS, k))
    for copy, when in sent:
        if when is None:
            copy.wait_send()
        else:
            pl.when(when)(copy.wait_send)


def place_kernel(blocks_ref, router_ref, down_out, router_out, sem, router_sem):
    copies = []
    for b in range(NZ):
        for k in range(CHUNKS):
            dst = down_out.at[pl.ds(b * CUT, CUT), pl.ds(k * LANES, LANES)]
            copies.append(pltpu.make_async_copy(blocks_ref.at[b, k], dst, sem.at[b, k]))
    copies.append(pltpu.make_async_copy(router_ref, router_out, router_sem))
    for copy in copies:
        copy.start()
    for copy in copies:
        copy.wait()


def on_device(train_down, router_weight, router_gain):
    anywhere = pl.BlockSpec(memory_space=pltpu.HBM)
    vmem = pl.BlockSpec(memory_space=pltpu.VMEM)
    owners = NY * NX * NC
    dma = pltpu.SemaphoreType.DMA
    blocks, router = pl.pallas_call(
        gather_kernel,
        name="gather",
        out_shape=(
            jax.ShapeDtypeStruct((NZ, CHUNKS, CUT, LANES), jnp.bfloat16),
            jax.ShapeDtypeStruct((owners, NZ * CUT), jnp.bfloat16),
        ),
        in_specs=[anywhere] * 3,
        out_specs=(vmem, vmem),
        scratch_shapes=[
            pltpu.VMEM((EXPERT, CUT), jnp.float32),
            pltpu.VMEM((2, LANES), jnp.float32),
            pltpu.VMEM((2, LANES), jnp.float32),
            pltpu.VMEM((NY, NX, NC, NZ, 2, LANES), jnp.float32),
            dma((CHUNKS,)),
            dma((2,)),
            pltpu.SemaphoreType.REGULAR((ROUNDS,)),
            dma((EVENTS,)), dma((EVENTS,)), dma((EVENTS,)), dma((EVENTS,)),
            dma((NZ - 1,)), dma((NZ - 1,)),
            dma((NY - 1,)), dma((NY - 1,)),
            dma((NX - 1,)), dma((NX - 1,)),
            dma, dma,
        ],
        compiler_params=pltpu.CompilerParams(
            collective_id=0, has_side_effects=True, vmem_limit_bytes=16 << 20
        ),
    )(
        *(pltpu.with_memory_space_constraint(array, pltpu.HBM) for array in (
            train_down.reshape(EXPERT, CUT),
            router_weight.reshape(2, LANES),
            router_gain.reshape(2, LANES),
        )),
    )
    ready, serve = pl.pallas_call(
        place_kernel,
        name="place",
        out_shape=(
            jax.ShapeDtypeStruct((NZ * CUT, EXPERT), jnp.bfloat16),
            jax.ShapeDtypeStruct((owners, NZ * CUT), jnp.bfloat16),
        ),
        in_specs=[vmem, vmem],
        out_specs=(anywhere, anywhere),
        scratch_shapes=[dma((NZ, CHUNKS)), dma],
        compiler_params=pltpu.CompilerParams(vmem_limit_bytes=16 << 20),
    )(blocks, router)
    return ready[None], serve.T


def solution(mesh):
    in_specs = (P("owner", None, "rows"), P("rows", "owner"), P("rows"))
    out_specs = (P("owner", None, None), P())
    return jax.shard_map(
        on_device, mesh=mesh, in_specs=in_specs, out_specs=out_specs, check_vma=False
    )
```

```python
import functools

import jax
import jax.numpy as jnp
from jax import lax
from jax.experimental import pallas as pl
from jax.experimental.pallas import tpu as pltpu
from jax.sharding import PartitionSpec as P

MESH = pl.DeviceIdType.MESH
NY, NX, NC, NZ = 8, 4, 2, 8
EXPERT = 1024
CUT = 256
LANES = 128
PIECES = EXPERT // LANES
GROUP = 1
CHUNKS = PIECES // GROUP
STEPS = NZ // 2 - 1
ROUNDS = 3
SHARE = (2, 4, 4, 4, 4, 4, 4, 6)
STAGES = (12, 19, 21, 23)
MEET, MEET_ROUNDS = 4, (6, 8, 10)
UP, DOWN, NORTH, SOUTH, EAST, WEST, TWIN = range(7)
BACK = (DOWN, UP, SOUTH, NORTH, WEST, EAST, TWIN)


def share_of(z):
    share = jnp.int32(SHARE[NZ - 1])
    for place in range(NZ - 1):
        share = jnp.where(z == place, jnp.int32(SHARE[place]), share)
    return share


def gather_kernel(
    down_ref, weight_ref, gain_ref,
    blocks_ref, router_ref,
    down, factors, columns,
    load_sem, small_sem, met_sem, along_sem, across_sem,
    send_sem, last_sem, recv_sem, recv_last,
    send_part, recv_part,
):
    owner = lax.axis_index("owner")
    z = lax.axis_index("rows")
    c = lax.rem(owner, NC)
    x = lax.rem(owner // NC, NX)
    y = owner // (NC * NX)

    edges = (1, 2, PIECES)
    loads = []
    for n, (low, high) in enumerate(zip((0, *edges), edges)):
        part = pl.ds(low * LANES, (high - low) * LANES)
        loads.append(pltpu.make_async_copy(down_ref.at[part], down.at[part], load_sem.at[n]))
    small = [
        pltpu.make_async_copy(weight_ref, factors.at[0], small_sem),
        pltpu.make_async_copy(gain_ref, factors.at[1], small_sem),
    ]
    loads[0].start()
    loads[1].start()
    small[0].start()
    small[1].start()
    loads[2].start()

    def device(yy, xx, cc, zz):
        return {"owner": (yy * NX + xx) * NC + cc, "rows": zz}

    def z_peer(d):
        return device(y, x, c, lax.rem(z + d, NZ))

    def y_peer(d):
        return device(lax.rem(y + d, NY), x, c, z)

    def x_peer(d):
        return device(y, lax.rem(x + d, NX), c, z)

    c_peer = device(y, x, NC - 1 - c, z)
    near = [z_peer(1), z_peer(NZ - 1), y_peer(1), y_peer(NY - 1), x_peer(1), x_peer(NX - 1)]
    near.append(c_peer)
    later = [
        z != NZ - 1, z == 0,
        y < NY // 2, jnp.logical_or(y > NY // 2, y == 0),
        x != NX - 1, x == 0,
        c == NC - 1,
    ]

    def tell(sem, peer):
        pl.semaphore_signal(sem, inc=1, device_id=peer, device_id_type=MESH)

    barrier = pltpu.get_barrier_semaphore()
    for peer, after in zip(near, later):
        pl.when(after)(functools.partial(tell, barrier, peer))
    earlier = sum(jnp.where(after, 0, 1) for after in later)

    def meet(i):
        pl.when(later[i])(lambda: pl.semaphore_wait(met_sem.at[i], 1))

    def met_at(i):
        return met_sem.at[min(BACK[i], NORTH)]

    share = share_of(z)
    share_above = share_of(lax.rem(z + 1, NZ))
    share_below = share_of(lax.rem(z + NZ - 1, NZ))

    def turn(k):
        piece = down[k * LANES : (k + 1) * LANES, :]
        blocks_ref[z, k] = jnp.transpose(piece).astype(jnp.bfloat16)

    def remote(ref, send, recv, peer):
        return pltpu.make_async_remote_copy(
            src_ref=ref, dst_ref=ref, send_sem=send, recv_sem=recv,
            device_id=peer, device_id_type=MESH,
        )

    def chunk_of(block, k):
        return blocks_ref.at[lax.rem(block, NZ), pl.ds(k * GROUP, GROUP)]

    def copy_up(step, k, block):
        return remote(chunk_of(block, k), send_sem, recv_sem.at[step * CHUNKS + k], near[UP])

    def copy_dn(step, k, block):
        return remote(chunk_of(block, k), send_sem, recv_sem.at[step * CHUNKS + k], near[DOWN])

    def end_up(k):
        slot = blocks_ref.at[lax.rem(z + NZ - STEPS, NZ), k]
        return remote(slot, last_sem.at[UP], recv_last, near[UP])

    def end_dn(k):
        slot = blocks_ref.at[lax.rem(z + STEPS, NZ), k]
        return remote(slot, last_sem.at[DOWN], recv_last, near[DOWN])

    def own_up(k):
        copy_up(0, k, z).start()

    def own_dn(k):
        copy_dn(0, k, z).start()

    pl.when(earlier > 0)(lambda: pl.semaphore_wait(barrier, earlier))
    for i, peer in enumerate(near):
        pl.when(jnp.logical_not(later[i]))(functools.partial(tell, met_at(i), peer))
    loads[0].wait()
    turn(0)
    loads[1].wait()
    turn(1)
    top, bottom = z == NZ - 1, z == 0
    ready = 2
    for k in range(CHUNKS):
        while ready < min((k + 1) * GROUP + 1, PIECES):
            if ready == 2:
                loads[2].wait()
            turn(ready)
            ready += 1
        pl.when(jnp.logical_not(bottom))(functools.partial(own_dn, k))
        pl.when(top)(functools.partial(own_up, k))
    meet(UP)
    for k in range(CHUNKS):
        pl.when(jnp.logical_not(top))(functools.partial(own_up, k))
    pltpu.make_async_copy(factors, factors, small_sem).wait()
    columns[y, x, c, z] = factors[0] * factors[1]
    meet(DOWN)
    for k in range(CHUNKS):
        pl.when(bottom)(functools.partial(own_dn, k))
    for r in range(ROUNDS):
        for peer in near[:NORTH]:
            tell(along_sem.at[r], peer)
        pl.semaphore_wait(along_sem.at[r], 2)

    def meet_across():
        count = sum(jnp.where(after, 1, 0) for after in later[NORTH:])
        pl.when(count > 0)(lambda: pl.semaphore_wait(met_sem.at[NORTH], count))
        for peer in near[NORTH:TWIN]:
            tell(across_sem.at[0], peer)

    def meet_round(r):
        pl.semaphore_wait(across_sem.at[r], 4)
        if r + 1 < ROUNDS:
            for peer in near[NORTH:TWIN]:
                tell(across_sem.at[r + 1], peer)

    def part(i, ref, peer):
        return remote(ref, send_part.at[i], recv_part.at[i], peer)

    own = columns.at[y, x, c, z]
    for d in range(1, NZ):
        part(0, own, z_peer(d)).start()

    def router_y():
        part(0, columns.at[y, x, c, pl.ds(0, NZ - 1)], z_peer(1)).wait_recv()
        for d in range(1, NY):
            part(1, columns.at[y, x, c], y_peer(d)).start()

    def router_x():
        part(1, columns.at[pl.ds(0, NY - 1), x, c], y_peer(1)).wait_recv()
        for d in range(1, NX):
            part(2, columns.at[:, x, c], x_peer(d)).start()

    def router_c():
        part(2, columns.at[:, pl.ds(0, NX - 1), c], x_peer(1)).wait_recv()
        part(3, columns.at[:, :, c], c_peer).start()

    def router_out():
        part(3, columns.at[:, :, NC - 1 - c], c_peer).wait_recv()
        for j in range(NZ * 2):
            piece = columns[:, :, :, j // 2, j % 2, :].reshape(NY * NX * NC, LANES)
            router_ref[:, j * LANES : (j + 1) * LANES] = piece.astype(jnp.bfloat16)

    stages = dict(zip(STAGES, (router_y, router_x, router_c, router_out)))
    stages[MEET] = meet_across
    stages.update((at, functools.partial(meet_round, r)) for r, at in enumerate(MEET_ROUNDS))
    for step in range(STEPS):
        for k in range(CHUNKS):
            both = blocks_ref.at[0, pl.ds(0, 2 * GROUP)]
            remote(both, send_sem, recv_sem.at[step * CHUNKS + k], near[UP]).wait_recv()
            if step + 1 < STEPS:
                copy_up(step + 1, k, z + NZ - step - 1).start()
                copy_dn(step + 1, k, z + step + 1).start()
            else:
                for n in range(k * GROUP, (k + 1) * GROUP):
                    if n < max(SHARE):
                        pl.when(n < share_above)(lambda n=n: end_up(n).start())
                    if n >= min(SHARE):
                        pl.when(n >= share_below)(lambda n=n: end_dn(n).start())
            for n in range(GROUP):
                if (step * CHUNKS + k) * GROUP + n in stages:
                    stages[(step * CHUNKS + k) * GROUP + n]()

    sent = blocks_ref.at[pl.ds(0, 2 * STEPS)]
    remote(sent, send_sem, recv_sem.at[0], near[UP]).wait_send()
    for n in sorted(set(SHARE)):
        up, dn = blocks_ref.at[0, pl.ds(0, n)], blocks_ref.at[0, pl.ds(n, PIECES - n)]
        pl.when(share_above == n)(remote(up, last_sem.at[UP], recv_last, near[UP]).wait_send)
        pl.when(share_below == n)(remote(dn, last_sem.at[DOWN], recv_last, near[DOWN]).wait_send)
    part(0, columns.at[y, x, c, pl.ds(0, NZ - 1)], z_peer(1)).wait_send()
    part(1, columns.at[pl.ds(0, NY - 1), x, c], y_peer(1)).wait_send()
    part(2, columns.at[:, pl.ds(0, NX - 1), c], x_peer(1)).wait_send()
    part(3, columns.at[:, :, c], c_peer).wait_send()
    far = blocks_ref.at[lax.rem(z + NZ // 2, NZ)]
    remote(far, last_sem.at[UP], recv_last, near[UP]).wait_recv()


def place_kernel(blocks_ref, router_ref, down_out, router_out, sem, router_sem):
    for b in range(NZ):
        for k in range(PIECES):
            dst = down_out.at[pl.ds(b * CUT, CUT), pl.ds(k * LANES, LANES)]
            pltpu.make_async_copy(blocks_ref.at[b, k], dst, sem).start()
    router = pltpu.make_async_copy(router_ref, router_out, router_sem)
    router.start()
    pltpu.make_async_copy(blocks_ref, blocks_ref, sem).wait()
    router.wait()


def on_device(train_down, router_weight, router_gain):
    hbm = pl.BlockSpec(memory_space=pltpu.HBM)
    vmem = pl.BlockSpec(memory_space=pltpu.VMEM)
    owners = NY * NX * NC
    dma, plain = pltpu.SemaphoreType.DMA, pltpu.SemaphoreType.REGULAR
    blocks, router = pl.pallas_call(
        gather_kernel,
        name="gather",
        out_shape=(
            jax.ShapeDtypeStruct((NZ, PIECES, CUT, LANES), jnp.bfloat16),
            jax.ShapeDtypeStruct((owners, NZ * CUT), jnp.bfloat16),
        ),
        in_specs=[hbm] * 3,
        out_specs=(vmem, vmem),
        scratch_shapes=[
            pltpu.VMEM((EXPERT, CUT), jnp.float32),
            pltpu.VMEM((2, 2, LANES), jnp.float32),
            pltpu.VMEM((NY, NX, NC, NZ, 2, LANES), jnp.float32),
            dma((3,)), dma, plain((NORTH + 1,)), plain((ROUNDS,)), plain((ROUNDS,)),
            dma, dma((2,)), dma((STEPS * CHUNKS,)), dma,
            dma((4,)), dma((4,)),
        ],
        compiler_params=pltpu.CompilerParams(
            collective_id=0, has_side_effects=True, vmem_limit_bytes=16 << 20
        ),
    )(
        *(pltpu.with_memory_space_constraint(array, pltpu.HBM) for array in (
            train_down.reshape(EXPERT, CUT),
            router_weight.reshape(2, LANES),
            router_gain.reshape(2, LANES),
        )),
    )
    ready, serve = pl.pallas_call(
        place_kernel,
        name="place",
        out_shape=(
            jax.ShapeDtypeStruct((NZ * CUT, EXPERT), jnp.bfloat16),
            jax.ShapeDtypeStruct((owners, NZ * CUT), jnp.bfloat16),
        ),
        in_specs=[vmem, vmem],
        out_specs=(hbm, hbm),
        scratch_shapes=[dma, dma],
        compiler_params=pltpu.CompilerParams(vmem_limit_bytes=16 << 20),
    )(blocks, router)
    return ready[None], serve.T


def solution(mesh):
    in_specs = (P("owner", None, "rows"), P("rows", "owner"), P("rows"))
    out_specs = (P("owner", None, None), P())
    return jax.shard_map(
        on_device, mesh=mesh, in_specs=in_specs, out_specs=out_specs, check_vma=False
    )
```

```python
import functools

import jax
import jax.numpy as jnp
from jax import lax
from jax.experimental import pallas as pl
from jax.experimental.pallas import tpu as pltpu
from jax.sharding import PartitionSpec as P

MESH = pl.DeviceIdType.MESH
NY, NX, NC, NZ = 8, 4, 2, 8
EXPERT = 1024
CUT = 256
LANES = 128
PIECES = EXPERT // LANES
GROUP = 1
CHUNKS = PIECES // GROUP
STEPS = NZ // 2 - 1
ROUNDS = 3
SHARE = (2, 4, 4, 4, 4, 4, 4, 6)
STAGES = (10, 15, 18, 20)
MEET, MEET_ROUNDS = 3, (5, 7, 9)
UP, DOWN, NORTH, SOUTH, EAST, WEST, TWIN = range(7)
BACK = (DOWN, UP, SOUTH, NORTH, WEST, EAST, TWIN)


def share_of(z):
    share = jnp.int32(SHARE[NZ - 1])
    for place in range(NZ - 1):
        share = jnp.where(z == place, jnp.int32(SHARE[place]), share)
    return share


def gather_kernel(
    down_ref, weight_ref, gain_ref,
    blocks_ref, router_ref,
    down, factors, columns,
    load_sem, small_sem, met_sem, along_sem, across_sem,
    send_sem, last_sem, recv_sem, recv_last,
    send_part, recv_part,
):
    owner = lax.axis_index("owner")
    z = lax.axis_index("rows")
    c = lax.rem(owner, NC)
    x = lax.rem(owner // NC, NX)
    y = owner // (NC * NX)

    edges = (1, 2, PIECES)
    loads = []
    for n, (low, high) in enumerate(zip((0, *edges), edges)):
        part = pl.ds(low * LANES, (high - low) * LANES)
        loads.append(pltpu.make_async_copy(down_ref.at[part], down.at[part], load_sem.at[n]))
    small = [
        pltpu.make_async_copy(weight_ref, factors.at[0], small_sem),
        pltpu.make_async_copy(gain_ref, factors.at[1], small_sem),
    ]
    loads[0].start()
    loads[1].start()
    small[0].start()
    small[1].start()
    loads[2].start()

    def device(yy, xx, cc, zz):
        return {"owner": (yy * NX + xx) * NC + cc, "rows": zz}

    def z_peer(d):
        return device(y, x, c, lax.rem(z + d, NZ))

    def y_peer(d):
        return device(lax.rem(y + d, NY), x, c, z)

    def x_peer(d):
        return device(y, lax.rem(x + d, NX), c, z)

    c_peer = device(y, x, NC - 1 - c, z)
    near = [z_peer(1), z_peer(NZ - 1), y_peer(1), y_peer(NY - 1), x_peer(1), x_peer(NX - 1)]
    near.append(c_peer)
    later = [
        z != NZ - 1, z == 0,
        y < NY // 2, jnp.logical_or(y > NY // 2, y == 0),
        x != NX - 1, x == 0,
        c == NC - 1,
    ]
    place = ((c * NZ + z) * NY + y) * NX + x
    first = place == 0
    for i, at in ((DOWN, NY * NX), (NORTH, (NY - 1) * NX), (SOUTH, NX), (EAST, NX - 1), (WEST, 1)):
        later[i] = jnp.logical_or(later[i], place == at)
    for i in (UP, NORTH, SOUTH, EAST, WEST):
        later[i] = jnp.logical_and(later[i], jnp.logical_not(first))

    def tell(sem, peer):
        pl.semaphore_signal(sem, inc=1, device_id=peer, device_id_type=MESH)

    barrier = pltpu.get_barrier_semaphore()
    for peer, after in zip(near, later):
        pl.when(after)(functools.partial(tell, barrier, peer))
    earlier = sum(jnp.where(after, 0, 1) for after in later)

    def meet(i):
        pl.when(later[i])(lambda: pl.semaphore_wait(met_sem.at[i], 1))

    def met_at(i):
        return met_sem.at[min(BACK[i], NORTH)]

    share = share_of(z)
    share_above = share_of(lax.rem(z + 1, NZ))
    share_below = share_of(lax.rem(z + NZ - 1, NZ))

    def turn(k):
        piece = down[k * LANES : (k + 1) * LANES, :]
        blocks_ref[z, k] = jnp.transpose(piece).astype(jnp.bfloat16)

    def remote(ref, send, recv, peer):
        return pltpu.make_async_remote_copy(
            src_ref=ref, dst_ref=ref, send_sem=send, recv_sem=recv,
            device_id=peer, device_id_type=MESH,
        )

    def chunk_of(block, k):
        return blocks_ref.at[lax.rem(block, NZ), pl.ds(k * GROUP, GROUP)]

    def copy_up(step, k, block):
        return remote(chunk_of(block, k), send_sem, recv_sem.at[step * CHUNKS + k], near[UP])

    def copy_dn(step, k, block):
        return remote(chunk_of(block, k), send_sem, recv_sem.at[step * CHUNKS + k], near[DOWN])

    def end_up(k):
        slot = blocks_ref.at[lax.rem(z + NZ - STEPS, NZ), k]
        return remote(slot, last_sem.at[UP], recv_last, near[UP])

    def end_dn(k):
        slot = blocks_ref.at[lax.rem(z + STEPS, NZ), k]
        return remote(slot, last_sem.at[DOWN], recv_last, near[DOWN])

    def own_up(k):
        copy_up(0, k, z).start()

    def own_dn(k):
        copy_dn(0, k, z).start()

    pl.when(earlier > 0)(lambda: pl.semaphore_wait(barrier, earlier))
    for i, peer in enumerate(near):
        pl.when(jnp.logical_not(later[i]))(functools.partial(tell, met_at(i), peer))
    loads[0].wait()
    turn(0)
    loads[1].wait()
    turn(1)
    ready = 2
    for k in range(CHUNKS):
        while ready < min((k + 1) * GROUP + 1, PIECES):
            if ready == 2:
                loads[2].wait()
            turn(ready)
            ready += 1
        pl.when(jnp.logical_not(later[DOWN]))(functools.partial(own_dn, k))
        pl.when(jnp.logical_not(later[UP]))(functools.partial(own_up, k))
    meet(UP)
    for k in range(CHUNKS):
        pl.when(later[UP])(functools.partial(own_up, k))
    pltpu.make_async_copy(factors, factors, small_sem).wait()
    columns[y, x, c, z] = factors[0] * factors[1]
    meet(DOWN)
    for k in range(CHUNKS):
        pl.when(later[DOWN])(functools.partial(own_dn, k))
    for r in range(ROUNDS):
        for peer in near[:NORTH]:
            tell(along_sem.at[r], peer)
        pl.semaphore_wait(along_sem.at[r], 2)

    def meet_across():
        count = sum(jnp.where(after, 1, 0) for after in later[NORTH:])
        pl.when(count > 0)(lambda: pl.semaphore_wait(met_sem.at[NORTH], count))
        for peer in near[NORTH:TWIN]:
            tell(across_sem.at[0], peer)

    def meet_round(r):
        pl.semaphore_wait(across_sem.at[r], 4)
        if r + 1 < ROUNDS:
            for peer in near[NORTH:TWIN]:
                tell(across_sem.at[r + 1], peer)

    def part(i, ref, peer):
        return remote(ref, send_part.at[i], recv_part.at[i], peer)

    own = columns.at[y, x, c, z]
    for d in range(1, NZ):
        part(0, own, z_peer(d)).start()

    def router_y():
        part(0, columns.at[y, x, c, pl.ds(0, NZ - 1)], z_peer(1)).wait_recv()
        for d in range(1, NY):
            part(1, columns.at[y, x, c], y_peer(d)).start()

    def router_x():
        part(1, columns.at[pl.ds(0, NY - 1), x, c], y_peer(1)).wait_recv()
        for d in range(1, NX):
            part(2, columns.at[:, x, c], x_peer(d)).start()

    def router_c():
        part(2, columns.at[:, pl.ds(0, NX - 1), c], x_peer(1)).wait_recv()
        part(3, columns.at[:, :, c], c_peer).start()

    def router_out():
        part(3, columns.at[:, :, NC - 1 - c], c_peer).wait_recv()
        for j in range(NZ * 2):
            piece = columns[:, :, :, j // 2, j % 2, :].reshape(NY * NX * NC, LANES)
            router_ref[:, j * LANES : (j + 1) * LANES] = piece.astype(jnp.bfloat16)

    stages = dict(zip(STAGES, (router_y, router_x, router_c, router_out)))
    stages[MEET] = meet_across
    stages.update((at, functools.partial(meet_round, r)) for r, at in enumerate(MEET_ROUNDS))
    for step in range(STEPS):
        for k in range(CHUNKS):
            both = blocks_ref.at[0, pl.ds(0, 2 * GROUP)]
            remote(both, send_sem, recv_sem.at[step * CHUNKS + k], near[UP]).wait_recv()
            if step + 1 < STEPS:
                copy_up(step + 1, k, z + NZ - step - 1).start()
                copy_dn(step + 1, k, z + step + 1).start()
            else:
                for n in range(k * GROUP, (k + 1) * GROUP):
                    if n < max(SHARE):
                        pl.when(n < share_above)(lambda n=n: end_up(n).start())
                    if n >= min(SHARE):
                        pl.when(n >= share_below)(lambda n=n: end_dn(n).start())
            for n in range(GROUP):
                if (step * CHUNKS + k) * GROUP + n in stages:
                    stages[(step * CHUNKS + k) * GROUP + n]()

    sent = blocks_ref.at[pl.ds(0, 2 * STEPS)]
    remote(sent, send_sem, recv_sem.at[0], near[UP]).wait_send()
    for n in sorted(set(SHARE)):
        up, dn = blocks_ref.at[0, pl.ds(0, n)], blocks_ref.at[0, pl.ds(n, PIECES - n)]
        pl.when(share_above == n)(remote(up, last_sem.at[UP], recv_last, near[UP]).wait_send)
        pl.when(share_below == n)(remote(dn, last_sem.at[DOWN], recv_last, near[DOWN]).wait_send)
    part(0, columns.at[y, x, c, pl.ds(0, NZ - 1)], z_peer(1)).wait_send()
    part(1, columns.at[pl.ds(0, NY - 1), x, c], y_peer(1)).wait_send()
    part(2, columns.at[:, pl.ds(0, NX - 1), c], x_peer(1)).wait_send()
    part(3, columns.at[:, :, c], c_peer).wait_send()
    far = blocks_ref.at[lax.rem(z + NZ // 2, NZ)]
    remote(far, last_sem.at[UP], recv_last, near[UP]).wait_recv()


def place_kernel(blocks_ref, router_ref, down_out, router_out, sem, router_sem):
    for b in range(NZ):
        for k in range(PIECES):
            dst = down_out.at[pl.ds(b * CUT, CUT), pl.ds(k * LANES, LANES)]
            pltpu.make_async_copy(blocks_ref.at[b, k], dst, sem).start()
    router = pltpu.make_async_copy(router_ref, router_out, router_sem)
    router.start()
    pltpu.make_async_copy(blocks_ref, blocks_ref, sem).wait()
    router.wait()


def on_device(train_down, router_weight, router_gain):
    hbm = pl.BlockSpec(memory_space=pltpu.HBM)
    vmem = pl.BlockSpec(memory_space=pltpu.VMEM)
    owners = NY * NX * NC
    dma, plain = pltpu.SemaphoreType.DMA, pltpu.SemaphoreType.REGULAR
    blocks, router = pl.pallas_call(
        gather_kernel,
        name="gather",
        out_shape=(
            jax.ShapeDtypeStruct((NZ, PIECES, CUT, LANES), jnp.bfloat16),
            jax.ShapeDtypeStruct((owners, NZ * CUT), jnp.bfloat16),
        ),
        in_specs=[hbm] * 3,
        out_specs=(vmem, vmem),
        scratch_shapes=[
            pltpu.VMEM((EXPERT, CUT), jnp.float32),
            pltpu.VMEM((2, 2, LANES), jnp.float32),
            pltpu.VMEM((NY, NX, NC, NZ, 2, LANES), jnp.float32),
            dma((3,)), dma, plain((NORTH + 1,)), plain((ROUNDS,)), plain((ROUNDS,)),
            dma, dma((2,)), dma((STEPS * CHUNKS,)), dma,
            dma((4,)), dma((4,)),
        ],
        compiler_params=pltpu.CompilerParams(
            collective_id=0, has_side_effects=True, vmem_limit_bytes=16 << 20
        ),
    )(
        *(pltpu.with_memory_space_constraint(array, pltpu.HBM) for array in (
            train_down.reshape(EXPERT, CUT),
            router_weight.reshape(2, LANES),
            router_gain.reshape(2, LANES),
        )),
    )
    ready, serve = pl.pallas_call(
        place_kernel,
        name="place",
        out_shape=(
            jax.ShapeDtypeStruct((NZ * CUT, EXPERT), jnp.bfloat16),
            jax.ShapeDtypeStruct((owners, NZ * CUT), jnp.bfloat16),
        ),
        in_specs=[vmem, vmem],
        out_specs=(hbm, hbm),
        scratch_shapes=[dma, dma],
        compiler_params=pltpu.CompilerParams(vmem_limit_bytes=16 << 20),
    )(blocks, router)
    return ready[None], serve.T


def solution(mesh):
    in_specs = (P("owner", None, "rows"), P("rows", "owner"), P("rows"))
    out_specs = (P("owner", None, None), P())
    return jax.shard_map(
        on_device, mesh=mesh, in_specs=in_specs, out_specs=out_specs, check_vma=False
    )
```

```python
import functools

import jax
import jax.numpy as jnp
from jax import lax
from jax.experimental import pallas as pl
from jax.experimental.pallas import tpu as pltpu
from jax.sharding import PartitionSpec as P

MESH = pl.DeviceIdType.MESH
NY, NX, NC, NZ = 8, 4, 2, 8
EXPERT = 1024
CUT = 256
LANES = 128
PIECES = EXPERT // LANES
GROUP = 2
CHUNKS = PIECES // GROUP
STEPS = NZ // 2 - 1
ROUNDS = 3
SHARE = ((1, 4, 4, 4, 4, 4, 4, 6), (2, 4, 4, 4, 4, 4, 4, 6))
CORNER_SHARE = 1
STAGES = (10, 15, 18, 20)
MEET, MEET_ROUNDS = 3, (5, 7, 9)
UP, DOWN, NORTH, SOUTH, EAST, WEST, TWIN = range(7)
BACK = (DOWN, UP, SOUTH, NORTH, WEST, EAST, TWIN)


def share_of(corner, c, z):
    share = jnp.int32(0)
    for core in range(NC):
        for place in range(NZ):
            share = jnp.where(jnp.logical_and(c == core, z == place), jnp.int32(SHARE[core][place]), share)
    at_start = jnp.logical_and(corner, jnp.logical_and(c == NC - 1, z == 0))
    return jnp.where(at_start, jnp.int32(CORNER_SHARE), share)


def gather_kernel(
    down_ref, weight_ref, gain_ref,
    blocks_ref, router_ref,
    down, factors, columns,
    load_sem, small_sem, met_sem, across_sem,
    send_sem, last_sem, recv_sem, recv_last,
    part_sem,
):
    owner = lax.axis_index("owner")
    z = lax.axis_index("rows")
    c = lax.rem(owner, NC)
    x = lax.rem(owner // NC, NX)
    y = owner // (NC * NX)

    edges = (2, PIECES)
    loads = []
    for n, (low, high) in enumerate(zip((0, *edges), edges)):
        part = pl.ds(low * LANES, (high - low) * LANES)
        loads.append(pltpu.make_async_copy(down_ref.at[part], down.at[part], load_sem.at[n]))
    small = [
        pltpu.make_async_copy(weight_ref, factors.at[0], small_sem),
        pltpu.make_async_copy(gain_ref, factors.at[1], small_sem),
    ]
    loads[0].start()
    small[0].start()
    small[1].start()
    loads[1].start()

    def device(yy, xx, cc, zz):
        return {"owner": (yy * NX + xx) * NC + cc, "rows": zz}

    def z_peer(d):
        return device(y, x, c, lax.rem(z + d, NZ))

    def y_peer(d):
        return device(lax.rem(y + d, NY), x, c, z)

    def x_peer(d):
        return device(y, lax.rem(x + d, NX), c, z)

    c_peer = device(y, x, NC - 1 - c, z)
    near = [z_peer(1), z_peer(NZ - 1), y_peer(1), y_peer(NY - 1), x_peer(1), x_peer(NX - 1)]
    near.append(c_peer)
    later = [
        z != NZ - 1, z == 0,
        y < NY // 2, jnp.logical_or(y > NY // 2, y == 0),
        x != NX - 1, x == 0,
        c == NC - 1,
    ]
    place = ((c * NZ + z) * NY + y) * NX + x
    first = place == 0
    for i, at in ((DOWN, NY * NX), (NORTH, (NY - 1) * NX), (SOUTH, NX), (EAST, NX - 1), (WEST, 1)):
        later[i] = jnp.logical_or(later[i], place == at)
    for i in (UP, NORTH, SOUTH, EAST, WEST):
        later[i] = jnp.logical_and(later[i], jnp.logical_not(first))

    def tell(sem, peer):
        pl.semaphore_signal(sem, inc=1, device_id=peer, device_id_type=MESH)

    barrier = pltpu.get_barrier_semaphore()
    for peer, after in zip(near, later):
        pl.when(after)(functools.partial(tell, barrier, peer))
    earlier = sum(jnp.where(after, 0, 1) for after in later)

    def meet(i):
        pl.when(later[i])(lambda: pl.semaphore_wait(met_sem.at[i], 1))

    def met_at(i):
        return met_sem.at[min(BACK[i], NORTH)]

    corner = jnp.logical_and(y == 0, x == 0)
    share_above = share_of(corner, c, lax.rem(z + 1, NZ))
    share_below = share_of(corner, c, lax.rem(z + NZ - 1, NZ))

    def comes_up(share, n):
        few = share <= PIECES // 2
        return jnp.logical_or(jnp.logical_and(few, n < share), jnp.logical_and(jnp.logical_not(few), n >= PIECES - share))


    def turn(k):
        piece = down[k * LANES : (k + 1) * LANES, :]
        blocks_ref[z, k] = jnp.transpose(piece).astype(jnp.bfloat16)

    def remote(ref, send, recv, peer):
        return pltpu.make_async_remote_copy(
            src_ref=ref, dst_ref=ref, send_sem=send, recv_sem=recv,
            device_id=peer, device_id_type=MESH,
        )

    def chunk_of(block, k):
        return blocks_ref.at[lax.rem(block, NZ), pl.ds(k * GROUP, GROUP)]

    def copy_up(step, k, block):
        return remote(chunk_of(block, k), send_sem, recv_sem.at[step * CHUNKS + k], near[UP])

    def copy_dn(step, k, block):
        return remote(chunk_of(block, k), send_sem, recv_sem.at[step * CHUNKS + k], near[DOWN])

    def end_up(k):
        slot = blocks_ref.at[lax.rem(z + NZ - STEPS, NZ), k]
        return remote(slot, last_sem.at[UP], recv_last, near[UP])

    def end_dn(k):
        slot = blocks_ref.at[lax.rem(z + STEPS, NZ), k]
        return remote(slot, last_sem.at[DOWN], recv_last, near[DOWN])

    def own_up(n):
        remote(blocks_ref.at[z, n], send_sem, recv_sem.at[n // GROUP], near[UP]).start()

    def own_dn(n):
        remote(blocks_ref.at[z, n], send_sem, recv_sem.at[n // GROUP], near[DOWN]).start()

    pl.when(earlier > 0)(lambda: pl.semaphore_wait(barrier, earlier))
    for i, peer in enumerate(near):
        pl.when(jnp.logical_not(later[i]))(functools.partial(tell, met_at(i), peer))
    loads[0].wait()
    turn(0)
    turn(1)
    for n in range(PIECES):
        if n == 1:
            loads[1].wait()
        if 1 <= n < PIECES - 1:
            turn(n + 1)
        pl.when(jnp.logical_not(later[DOWN]))(functools.partial(own_dn, n))
        pl.when(jnp.logical_not(later[UP]))(functools.partial(own_up, n))
    meet(UP)
    for n in range(PIECES):
        pl.when(later[UP])(functools.partial(own_up, n))
    pltpu.make_async_copy(factors, factors, small_sem).wait()
    columns[y, x, c, z] = factors[0] * factors[1]
    meet(DOWN)
    for n in range(PIECES):
        pl.when(later[DOWN])(functools.partial(own_dn, n))
    for _ in range(ROUNDS):
        for i in (UP, DOWN):
            tell(met_at(i), near[i])
        for i in (UP, DOWN):
            pl.semaphore_wait(met_sem.at[i], 1)

    def meet_across():
        count = sum(jnp.where(after, 1, 0) for after in later[NORTH:])
        pl.when(count > 0)(lambda: pl.semaphore_wait(met_sem.at[NORTH], count))
        for peer in near[NORTH:TWIN]:
            tell(across_sem.at[0], peer)

    def meet_round(r):
        pl.semaphore_wait(across_sem.at[r], 4)
        if r + 1 < ROUNDS:
            for peer in near[NORTH:TWIN]:
                tell(across_sem.at[r + 1], peer)

    def part(i, ref, peer):
        return remote(ref, part_sem.at[i], part_sem.at[i], peer)

    own = columns.at[y, x, c, z]
    for d in range(1, NZ):
        part(0, own, z_peer(d)).start()

    def router_y():
        part(0, columns.at[y, x, :, pl.ds(0, NZ - 1)], z_peer(1)).wait_recv()
        for d in range(1, NY):
            part(1, columns.at[y, x, c], y_peer(d)).start()

    def router_x():
        part(1, columns.at[pl.ds(0, NY - 1), x], y_peer(1)).wait_recv()
        for d in range(1, NX):
            part(2, columns.at[:, x, c], x_peer(d)).start()

    def router_c():
        part(2, columns.at[:, pl.ds(0, NX - 1)], x_peer(1)).wait_recv()
        part(3, columns.at[:, :, c], c_peer).start()

    def router_out():
        part(3, columns, c_peer).wait_recv()
        for j in range(NZ * 2):
            piece = columns[:, :, :, j // 2, j % 2, :].reshape(NY * NX * NC, LANES)
            router_ref[:, j * LANES : (j + 1) * LANES] = piece.astype(jnp.bfloat16)

    feeder = z == 1
    stages = dict(zip(STAGES, (router_y, router_x)))
    for at, stage in zip(STAGES[2:], (router_c, router_out)):
        stages[at] = functools.partial(pl.when(jnp.logical_not(feeder)), stage)
    stages[MEET] = meet_across
    stages.update((at, functools.partial(meet_round, r)) for r, at in enumerate(MEET_ROUNDS))
    for step in range(STEPS):
        for k in range(CHUNKS):
            both = blocks_ref.at[0, pl.ds(0, 2 * GROUP)]
            remote(both, send_sem, recv_sem.at[step * CHUNKS + k], near[UP]).wait_recv()
            if step + 1 < STEPS:
                copy_up(step + 1, k, z + NZ - step - 1).start()
                copy_dn(step + 1, k, z + step + 1).start()
            else:
                for n in range(k * GROUP, (k + 1) * GROUP):
                    pl.when(comes_up(share_above, n))(lambda n=n: end_up(n).start())
                    pl.when(jnp.logical_not(comes_up(share_below, n)))(lambda n=n: end_dn(n).start())
            for n in range(GROUP):
                if (step * CHUNKS + k) * GROUP + n in stages:
                    stages[(step * CHUNKS + k) * GROUP + n]()

    @pl.when(feeder)
    def _():
        router_c()
        router_out()

    sent = blocks_ref.at[pl.ds(0, 2 * STEPS)]
    remote(sent, send_sem, recv_sem.at[0], near[UP]).wait_send()
    for n in sorted({*SHARE[0], *SHARE[1], CORNER_SHARE}):
        if n > 0:
            up = blocks_ref.at[0, pl.ds(0, n)]
            pl.when(share_above == n)(remote(up, last_sem.at[UP], recv_last, near[UP]).wait_send)
        if n < PIECES:
            dn = blocks_ref.at[0, pl.ds(0, PIECES - n)]
            pl.when(share_below == n)(remote(dn, last_sem.at[DOWN], recv_last, near[DOWN]).wait_send)
    far = blocks_ref.at[lax.rem(z + NZ // 2, NZ)]
    remote(far, last_sem.at[UP], recv_last, near[UP]).wait_recv()


def place_kernel(blocks_ref, router_ref, down_out, router_out, sem, router_sem):
    for b in range(NZ):
        for k in range(PIECES):
            dst = down_out.at[pl.ds(b * CUT, CUT), pl.ds(k * LANES, LANES)]
            pltpu.make_async_copy(blocks_ref.at[b, k], dst, sem).start()
    router = pltpu.make_async_copy(router_ref, router_out, router_sem)
    router.start()
    pltpu.make_async_copy(blocks_ref, blocks_ref, sem).wait()
    router.wait()


def on_device(train_down, router_weight, router_gain):
    hbm = pl.BlockSpec(memory_space=pltpu.HBM)
    vmem = pl.BlockSpec(memory_space=pltpu.VMEM)
    owners = NY * NX * NC
    dma, plain = pltpu.SemaphoreType.DMA, pltpu.SemaphoreType.REGULAR
    blocks, router = pl.pallas_call(
        gather_kernel,
        name="gather",
        out_shape=(
            jax.ShapeDtypeStruct((NZ, PIECES, CUT, LANES), jnp.bfloat16),
            jax.ShapeDtypeStruct((owners, NZ * CUT), jnp.bfloat16),
        ),
        in_specs=[hbm] * 3,
        out_specs=(vmem, vmem),
        scratch_shapes=[
            pltpu.VMEM((EXPERT, CUT), jnp.float32),
            pltpu.VMEM((2, 2, LANES), jnp.float32),
            pltpu.VMEM((NY, NX, NC, NZ, 2, LANES), jnp.float32),
            dma((2,)), dma, plain((NORTH + 1,)), plain((ROUNDS,)),
            dma, dma((2,)), dma((STEPS * CHUNKS,)), dma,
            dma((4,)),
        ],
        compiler_params=pltpu.CompilerParams(
            collective_id=0, has_side_effects=True, vmem_limit_bytes=16 << 20
        ),
    )(
        *(pltpu.with_memory_space_constraint(array, pltpu.HBM) for array in (
            train_down.reshape(EXPERT, CUT),
            router_weight.reshape(2, LANES),
            router_gain.reshape(2, LANES),
        )),
    )
    ready, serve = pl.pallas_call(
        place_kernel,
        name="place",
        out_shape=(
            jax.ShapeDtypeStruct((NZ * CUT, EXPERT), jnp.bfloat16),
            jax.ShapeDtypeStruct((owners, NZ * CUT), jnp.bfloat16),
        ),
        in_specs=[vmem, vmem],
        out_specs=(hbm, hbm),
        scratch_shapes=[dma, dma],
        compiler_params=pltpu.CompilerParams(vmem_limit_bytes=16 << 20),
    )(blocks, router)
    return ready[None], serve.T


def solution(mesh):
    in_specs = (P("owner", None, "rows"), P("rows", "owner"), P("rows"))
    out_specs = (P("owner", None, None), P())
    return jax.shard_map(
        on_device, mesh=mesh, in_specs=in_specs, out_specs=out_specs, check_vma=False
    )
```

```python
import functools

import jax
import jax.numpy as jnp
from jax import lax
from jax.experimental import pallas as pl
from jax.experimental.pallas import tpu as pltpu
from jax.sharding import PartitionSpec as P

MESH = pl.DeviceIdType.MESH
NY, NX, NC, NZ = 8, 4, 2, 8
EXPERT = 1024
CUT = 256
LANES = 128
PIECES = EXPERT // LANES
GROUP = 2
CHUNKS = PIECES // GROUP
STEPS = NZ // 2 - 1
ROUNDS = 3
SHARE = ((1, 4, 4, 4, 4, 4, 4, 6), (2, 4, 4, 4, 4, 4, 4, 6))
CORNER_SHARE = 1
STAGES = (10, 15, 18, 20)
MEET, MEET_ROUNDS = 3, (5, 7, 9)
AHEAD = 2
UP, DOWN, NORTH, SOUTH, EAST, WEST, TWIN = range(7)
BACK = (DOWN, UP, SOUTH, NORTH, WEST, EAST, TWIN)


def share_of(corner, c, z):
    share = jnp.int32(0)
    for core in range(NC):
        for place in range(NZ):
            share = jnp.where(jnp.logical_and(c == core, z == place), jnp.int32(SHARE[core][place]), share)
    at_start = jnp.logical_and(corner, jnp.logical_and(c == NC - 1, z == 0))
    return jnp.where(at_start, jnp.int32(CORNER_SHARE), share)


def gather_kernel(
    down_ref, weight_ref, gain_ref,
    blocks_ref, router_ref,
    down, factors, columns,
    load_sem, small_sem, met_sem, across_sem,
    send_sem, last_sem, recv_sem, recv_last,
    part_sem,
):
    owner = lax.axis_index("owner")
    z = lax.axis_index("rows")
    c = lax.rem(owner, NC)
    x = lax.rem(owner // NC, NX)
    y = owner // (NC * NX)

    edges = (2, PIECES)
    loads = []
    for n, (low, high) in enumerate(zip((0, *edges), edges)):
        part = pl.ds(low * LANES, (high - low) * LANES)
        loads.append(pltpu.make_async_copy(down_ref.at[part], down.at[part], load_sem.at[n]))
    small = [
        pltpu.make_async_copy(weight_ref, factors.at[0], small_sem),
        pltpu.make_async_copy(gain_ref, factors.at[1], small_sem),
    ]
    loads[0].start()
    small[0].start()
    small[1].start()
    loads[1].start()

    def device(yy, xx, cc, zz):
        return {"owner": (yy * NX + xx) * NC + cc, "rows": zz}

    def z_peer(d):
        return device(y, x, c, lax.rem(z + d, NZ))

    def y_peer(d):
        return device(lax.rem(y + d, NY), x, c, z)

    def x_peer(d):
        return device(y, lax.rem(x + d, NX), c, z)

    c_peer = device(y, x, NC - 1 - c, z)
    near = [z_peer(1), z_peer(NZ - 1), y_peer(1), y_peer(NY - 1), x_peer(1), x_peer(NX - 1)]
    near.append(c_peer)
    later = [
        z != NZ - 1, z == 0,
        y < NY // 2, jnp.logical_or(y > NY // 2, y == 0),
        x != NX - 1, x == 0,
        c == NC - 1,
    ]
    place = ((c * NZ + z) * NY + y) * NX + x
    first = place == 0
    for i, at in ((DOWN, NY * NX), (NORTH, (NY - 1) * NX), (SOUTH, NX), (EAST, NX - 1), (WEST, 1)):
        later[i] = jnp.logical_or(later[i], place == at)
    for i in (UP, NORTH, SOUTH, EAST, WEST):
        later[i] = jnp.logical_and(later[i], jnp.logical_not(first))

    def tell(sem, peer):
        pl.semaphore_signal(sem, inc=1, device_id=peer, device_id_type=MESH)

    barrier = pltpu.get_barrier_semaphore()
    for peer, after in zip(near, later):
        pl.when(after)(functools.partial(tell, barrier, peer))
    earlier = sum(jnp.where(after, 0, 1) for after in later)

    def meet(i):
        pl.when(later[i])(lambda: pl.semaphore_wait(met_sem.at[i], 1))

    def met_at(i):
        return met_sem.at[min(BACK[i], NORTH)]

    corner = jnp.logical_and(y == 0, x == 0)
    share_above = share_of(corner, c, lax.rem(z + 1, NZ))
    share_below = share_of(corner, c, lax.rem(z + NZ - 1, NZ))

    def comes_up(share, n):
        few = share <= PIECES // 2
        return jnp.logical_or(jnp.logical_and(few, n < share), jnp.logical_and(jnp.logical_not(few), n >= PIECES - share))


    def turn(k):
        piece = down[k * LANES : (k + 1) * LANES, :]
        blocks_ref[z, k] = jnp.transpose(piece).astype(jnp.bfloat16)

    def remote(ref, send, recv, peer):
        return pltpu.make_async_remote_copy(
            src_ref=ref, dst_ref=ref, send_sem=send, recv_sem=recv,
            device_id=peer, device_id_type=MESH,
        )

    def chunk_of(block, k):
        return blocks_ref.at[lax.rem(block, NZ), pl.ds(k * GROUP, GROUP)]

    def copy_up(step, k, block):
        return remote(chunk_of(block, k), send_sem, recv_sem.at[step * CHUNKS + k], near[UP])

    def copy_dn(step, k, block):
        return remote(chunk_of(block, k), send_sem, recv_sem.at[step * CHUNKS + k], near[DOWN])

    def end_up(k):
        slot = blocks_ref.at[lax.rem(z + NZ - STEPS, NZ), k]
        return remote(slot, last_sem.at[UP], recv_last, near[UP])

    def end_dn(k):
        slot = blocks_ref.at[lax.rem(z + STEPS, NZ), k]
        return remote(slot, last_sem.at[DOWN], recv_last, near[DOWN])

    def own_up(n):
        remote(blocks_ref.at[z, n], send_sem, recv_sem.at[n // GROUP], near[UP]).start()

    def own_dn(n):
        remote(blocks_ref.at[z, n], send_sem, recv_sem.at[n // GROUP], near[DOWN]).start()

    pl.when(earlier > 0)(lambda: pl.semaphore_wait(barrier, earlier))
    for i, peer in enumerate(near):
        pl.when(jnp.logical_not(later[i]))(functools.partial(tell, met_at(i), peer))
    loads[0].wait()
    turn(0)
    turn(1)
    for n in range(PIECES):
        if n == 1:
            loads[1].wait()
        if 1 <= n < PIECES - 1:
            turn(n + 1)
        pl.when(jnp.logical_not(later[DOWN]))(functools.partial(own_dn, n))
        pl.when(jnp.logical_not(later[UP]))(functools.partial(own_up, n))
    meet(UP)
    for n in range(PIECES):
        pl.when(later[UP])(functools.partial(own_up, n))
    pltpu.make_async_copy(factors, factors, small_sem).wait()
    columns[y, x, c, z] = factors[0] * factors[1]
    meet(DOWN)
    for n in range(PIECES):
        pl.when(later[DOWN])(functools.partial(own_dn, n))
    def forward(step, k):
        both = blocks_ref.at[0, pl.ds(0, 2 * GROUP)]
        remote(both, send_sem, recv_sem.at[step * CHUNKS + k], near[UP]).wait_recv()
        if step + 1 < STEPS:
            copy_up(step + 1, k, z + NZ - step - 1).start()
            copy_dn(step + 1, k, z + step + 1).start()
        else:
            for n in range(k * GROUP, (k + 1) * GROUP):
                pl.when(comes_up(share_above, n))(lambda n=n: end_up(n).start())
                pl.when(jnp.logical_not(comes_up(share_below, n)))(lambda n=n: end_dn(n).start())

    feeder = z == 1
    for k in range(AHEAD):
        pl.when(feeder)(functools.partial(forward, 0, k))
    for _ in range(ROUNDS):
        for i in (UP, DOWN):
            tell(met_at(i), near[i])
        for i in (UP, DOWN):
            pl.semaphore_wait(met_sem.at[i], 1)

    def meet_across():
        count = sum(jnp.where(after, 1, 0) for after in later[NORTH:])
        pl.when(count > 0)(lambda: pl.semaphore_wait(met_sem.at[NORTH], count))
        for peer in near[NORTH:TWIN]:
            tell(across_sem.at[0], peer)

    def meet_round(r):
        pl.semaphore_wait(across_sem.at[r], 4)
        if r + 1 < ROUNDS:
            for peer in near[NORTH:TWIN]:
                tell(across_sem.at[r + 1], peer)

    def part(i, ref, peer):
        return remote(ref, part_sem.at[i], part_sem.at[i], peer)

    own = columns.at[y, x, c, z]
    for d in range(1, NZ):
        part(0, own, z_peer(d)).start()

    def router_y():
        part(0, columns.at[y, x, :, pl.ds(0, NZ - 1)], z_peer(1)).wait_recv()
        for d in range(1, NY):
            part(1, columns.at[y, x, c], y_peer(d)).start()

    def router_x():
        part(1, columns.at[pl.ds(0, NY - 1), x], y_peer(1)).wait_recv()
        for d in range(1, NX):
            part(2, columns.at[:, x, c], x_peer(d)).start()

    def router_c():
        part(2, columns.at[:, pl.ds(0, NX - 1)], x_peer(1)).wait_recv()
        part(3, columns.at[:, :, c], c_peer).start()

    def router_out():
        part(3, columns, c_peer).wait_recv()
        for j in range(NZ * 2):
            piece = columns[:, :, :, j // 2, j % 2, :].reshape(NY * NX * NC, LANES)
            router_ref[:, j * LANES : (j + 1) * LANES] = piece.astype(jnp.bfloat16)

    stages = dict(zip(STAGES, (router_y, router_x)))
    for at, stage in zip(STAGES[2:], (router_c, router_out)):
        stages[at] = functools.partial(pl.when(jnp.logical_not(feeder)), stage)
    stages[MEET] = meet_across
    stages.update((at, functools.partial(meet_round, r)) for r, at in enumerate(MEET_ROUNDS))
    for step in range(STEPS):
        for k in range(CHUNKS):
            if step * CHUNKS + k < AHEAD:
                pl.when(jnp.logical_not(feeder))(functools.partial(forward, step, k))
            else:
                forward(step, k)
            for n in range(GROUP):
                if (step * CHUNKS + k) * GROUP + n in stages:
                    stages[(step * CHUNKS + k) * GROUP + n]()

    @pl.when(feeder)
    def _():
        router_c()
        router_out()

    sent = blocks_ref.at[pl.ds(0, 2 * STEPS)]
    remote(sent, send_sem, recv_sem.at[0], near[UP]).wait_send()
    for n in sorted({*SHARE[0], *SHARE[1], CORNER_SHARE}):
        if n > 0:
            up = blocks_ref.at[0, pl.ds(0, n)]
            pl.when(share_above == n)(remote(up, last_sem.at[UP], recv_last, near[UP]).wait_send)
        if n < PIECES:
            dn = blocks_ref.at[0, pl.ds(0, PIECES - n)]
            pl.when(share_below == n)(remote(dn, last_sem.at[DOWN], recv_last, near[DOWN]).wait_send)
    far = blocks_ref.at[lax.rem(z + NZ // 2, NZ)]
    remote(far, last_sem.at[UP], recv_last, near[UP]).wait_recv()


def place_kernel(blocks_ref, router_ref, down_out, router_out, sem, router_sem):
    for b in range(NZ):
        for k in range(PIECES):
            dst = down_out.at[pl.ds(b * CUT, CUT), pl.ds(k * LANES, LANES)]
            pltpu.make_async_copy(blocks_ref.at[b, k], dst, sem).start()
    router = pltpu.make_async_copy(router_ref, router_out, router_sem)
    router.start()
    pltpu.make_async_copy(blocks_ref, blocks_ref, sem).wait()
    router.wait()


def on_device(train_down, router_weight, router_gain):
    hbm = pl.BlockSpec(memory_space=pltpu.HBM)
    vmem = pl.BlockSpec(memory_space=pltpu.VMEM)
    owners = NY * NX * NC
    dma, plain = pltpu.SemaphoreType.DMA, pltpu.SemaphoreType.REGULAR
    blocks, router = pl.pallas_call(
        gather_kernel,
        name="gather",
        out_shape=(
            jax.ShapeDtypeStruct((NZ, PIECES, CUT, LANES), jnp.bfloat16),
            jax.ShapeDtypeStruct((owners, NZ * CUT), jnp.bfloat16),
        ),
        in_specs=[hbm] * 3,
        out_specs=(vmem, vmem),
        scratch_shapes=[
            pltpu.VMEM((EXPERT, CUT), jnp.float32),
            pltpu.VMEM((2, 2, LANES), jnp.float32),
            pltpu.VMEM((NY, NX, NC, NZ, 2, LANES), jnp.float32),
            dma((2,)), dma, plain((NORTH + 1,)), plain((ROUNDS,)),
            dma, dma((2,)), dma((STEPS * CHUNKS,)), dma,
            dma((4,)),
        ],
        compiler_params=pltpu.CompilerParams(
            collective_id=0, has_side_effects=True, vmem_limit_bytes=16 << 20
        ),
    )(
        *(pltpu.with_memory_space_constraint(array, pltpu.HBM) for array in (
            train_down.reshape(EXPERT, CUT),
            router_weight.reshape(2, LANES),
            router_gain.reshape(2, LANES),
        )),
    )
    ready, serve = pl.pallas_call(
        place_kernel,
        name="place",
        out_shape=(
            jax.ShapeDtypeStruct((NZ * CUT, EXPERT), jnp.bfloat16),
            jax.ShapeDtypeStruct((owners, NZ * CUT), jnp.bfloat16),
        ),
        in_specs=[vmem, vmem],
        out_specs=(hbm, hbm),
        scratch_shapes=[dma, dma],
        compiler_params=pltpu.CompilerParams(vmem_limit_bytes=16 << 20),
    )(blocks, router)
    return ready[None], serve.T


def solution(mesh):
    in_specs = (P("owner", None, "rows"), P("rows", "owner"), P("rows"))
    out_specs = (P("owner", None, None), P())
    return jax.shard_map(
        on_device, mesh=mesh, in_specs=in_specs, out_specs=out_specs, check_vma=False
    )
```

```python
import functools

import jax
import jax.numpy as jnp
from jax import lax
from jax.experimental import pallas as pl
from jax.experimental.pallas import tpu as pltpu
from jax.sharding import PartitionSpec as P

MESH = pl.DeviceIdType.MESH
NY, NX, NC, NZ = 8, 4, 2, 8
EXPERT = 1024
CUT = 256
LANES = 128
PIECES = EXPERT // LANES
GROUP = 2
CHUNKS = PIECES // GROUP
STEPS = NZ // 2 - 1
ROUNDS = 3
SHARE = ((1, 4, 4, 4, 4, 4, 4, 6), (2, 4, 4, 4, 4, 4, 4, 6))
CORNER_SHARE = 1
STAGES = (8, 10, 15, 18, 20)
MEET, MEET_ROUNDS = 3, (5, 7, 9)
AHEAD = 2
UP, DOWN, NORTH, SOUTH, EAST, WEST, TWIN = range(7)
BACK = (DOWN, UP, SOUTH, NORTH, WEST, EAST, TWIN)


def share_of(corner, c, z):
    share = jnp.int32(0)
    for core in range(NC):
        for place in range(NZ):
            share = jnp.where(jnp.logical_and(c == core, z == place), jnp.int32(SHARE[core][place]), share)
    at_start = jnp.logical_and(corner, jnp.logical_and(c == NC - 1, z == 0))
    return jnp.where(at_start, jnp.int32(CORNER_SHARE), share)


def gather_kernel(
    down_ref, weight_ref, gain_ref,
    blocks_ref, router_ref,
    down, factors, rounded, columns,
    load_sem, small_sem, met_sem, across_sem,
    send_sem, last_sem, recv_sem, recv_last,
    part_sem,
):
    owner = lax.axis_index("owner")
    z = lax.axis_index("rows")
    c = lax.rem(owner, NC)
    x = lax.rem(owner // NC, NX)
    y = owner // (NC * NX)

    edges = (2, PIECES)
    loads = []
    for n, (low, high) in enumerate(zip((0, *edges), edges)):
        part = pl.ds(low * LANES, (high - low) * LANES)
        loads.append(pltpu.make_async_copy(down_ref.at[part], down.at[part], load_sem.at[n]))
    small = [
        pltpu.make_async_copy(weight_ref, factors.at[0], small_sem),
        pltpu.make_async_copy(gain_ref, factors.at[1], small_sem),
    ]
    loads[0].start()
    small[0].start()
    small[1].start()
    loads[1].start()

    def device(yy, xx, cc, zz):
        return {"owner": (yy * NX + xx) * NC + cc, "rows": zz}

    def z_peer(d):
        return device(y, x, c, lax.rem(z + d, NZ))

    def y_peer(d):
        return device(lax.rem(y + d, NY), x, c, z)

    def x_peer(d):
        return device(y, lax.rem(x + d, NX), c, z)

    c_peer = device(y, x, NC - 1 - c, z)
    near = [z_peer(1), z_peer(NZ - 1), y_peer(1), y_peer(NY - 1), x_peer(1), x_peer(NX - 1)]
    near.append(c_peer)
    later = [
        z != NZ - 1, z == 0,
        y < NY // 2, jnp.logical_or(y > NY // 2, y == 0),
        x != NX - 1, x == 0,
        c == NC - 1,
    ]
    place = ((c * NZ + z) * NY + y) * NX + x
    first = place == 0
    for i, at in ((DOWN, NY * NX), (NORTH, (NY - 1) * NX), (SOUTH, NX), (EAST, NX - 1), (WEST, 1)):
        later[i] = jnp.logical_or(later[i], place == at)
    for i in (UP, NORTH, SOUTH, EAST, WEST):
        later[i] = jnp.logical_and(later[i], jnp.logical_not(first))

    def tell(sem, peer):
        pl.semaphore_signal(sem, inc=1, device_id=peer, device_id_type=MESH)

    barrier = pltpu.get_barrier_semaphore()
    for peer, after in zip(near, later):
        pl.when(after)(functools.partial(tell, barrier, peer))
    earlier = sum(jnp.where(after, 0, 1) for after in later)

    def meet(i):
        pl.when(later[i])(lambda: pl.semaphore_wait(met_sem.at[i], 1))

    def met_at(i):
        return met_sem.at[min(BACK[i], NORTH)]

    corner = jnp.logical_and(y == 0, x == 0)
    share_above = share_of(corner, c, lax.rem(z + 1, NZ))
    share_below = share_of(corner, c, lax.rem(z + NZ - 1, NZ))

    def comes_up(share, n):
        few = share <= PIECES // 2
        return jnp.logical_or(jnp.logical_and(few, n < share), jnp.logical_and(jnp.logical_not(few), n >= PIECES - share))


    def turn(k):
        piece = down[k * LANES : (k + 1) * LANES, :]
        blocks_ref[z, k] = jnp.transpose(piece).astype(jnp.bfloat16)

    def remote(ref, send, recv, peer):
        return pltpu.make_async_remote_copy(
            src_ref=ref, dst_ref=ref, send_sem=send, recv_sem=recv,
            device_id=peer, device_id_type=MESH,
        )

    def chunk_of(block, k):
        return blocks_ref.at[lax.rem(block, NZ), pl.ds(k * GROUP, GROUP)]

    def copy_up(step, k, block):
        return remote(chunk_of(block, k), send_sem, recv_sem.at[step * CHUNKS + k], near[UP])

    def copy_dn(step, k, block):
        return remote(chunk_of(block, k), send_sem, recv_sem.at[step * CHUNKS + k], near[DOWN])

    def end_up(k):
        slot = blocks_ref.at[lax.rem(z + NZ - STEPS, NZ), k]
        return remote(slot, last_sem.at[UP], recv_last, near[UP])

    def end_dn(k):
        slot = blocks_ref.at[lax.rem(z + STEPS, NZ), k]
        return remote(slot, last_sem.at[DOWN], recv_last, near[DOWN])

    def own_up(n):
        remote(blocks_ref.at[z, n], send_sem, recv_sem.at[n // GROUP], near[UP]).start()

    def own_dn(n):
        remote(blocks_ref.at[z, n], send_sem, recv_sem.at[n // GROUP], near[DOWN]).start()

    pl.when(earlier > 0)(lambda: pl.semaphore_wait(barrier, earlier))
    for i, peer in enumerate(near):
        pl.when(jnp.logical_not(later[i]))(functools.partial(tell, met_at(i), peer))
    loads[0].wait()
    turn(0)
    turn(1)
    for n in range(PIECES):
        if n == 1:
            loads[1].wait()
        if 1 <= n < PIECES - 1:
            turn(n + 1)
        pl.when(jnp.logical_not(later[DOWN]))(functools.partial(own_dn, n))
        pl.when(jnp.logical_not(later[UP]))(functools.partial(own_up, n))
    meet(UP)
    for n in range(PIECES):
        pl.when(later[UP])(functools.partial(own_up, n))
    pltpu.make_async_copy(factors, factors, small_sem).wait()
    rounded[z] = (factors[0] * factors[1]).astype(jnp.bfloat16)
    meet(DOWN)
    for n in range(PIECES):
        pl.when(later[DOWN])(functools.partial(own_dn, n))
    def forward(step, k):
        both = blocks_ref.at[0, pl.ds(0, 2 * GROUP)]
        remote(both, send_sem, recv_sem.at[step * CHUNKS + k], near[UP]).wait_recv()
        if step + 1 < STEPS:
            copy_up(step + 1, k, z + NZ - step - 1).start()
            copy_dn(step + 1, k, z + step + 1).start()
        else:
            for n in range(k * GROUP, (k + 1) * GROUP):
                pl.when(comes_up(share_above, n))(lambda n=n: end_up(n).start())
                pl.when(jnp.logical_not(comes_up(share_below, n)))(lambda n=n: end_dn(n).start())

    feeder = z == 1
    for k in range(AHEAD):
        pl.when(feeder)(functools.partial(forward, 0, k))
    for _ in range(ROUNDS):
        for i in (UP, DOWN):
            tell(met_at(i), near[i])
        for i in (UP, DOWN):
            pl.semaphore_wait(met_sem.at[i], 1)

    def meet_across():
        count = sum(jnp.where(after, 1, 0) for after in later[NORTH:])
        pl.when(count > 0)(lambda: pl.semaphore_wait(met_sem.at[NORTH], count))
        for peer in near[NORTH:TWIN]:
            tell(across_sem.at[0], peer)

    def meet_round(r):
        pl.semaphore_wait(across_sem.at[r], 4)
        if r + 1 < ROUNDS:
            for peer in near[NORTH:TWIN]:
                tell(across_sem.at[r + 1], peer)

    def part(i, ref, peer):
        return remote(ref, part_sem.at[i], part_sem.at[i], peer)

    own = rounded.at[z]
    for d in range(1, NZ):
        part(0, own, z_peer(d)).start()

    def router_z():
        part(0, columns.at[y, x, c, pl.ds(0, NZ - 1)], z_peer(1)).wait_recv()
        columns[y, x, c] = rounded[...].astype(jnp.float32)

    def router_y():
        for d in range(1, NY):
            part(1, columns.at[y, x, c], y_peer(d)).start()

    def router_x():
        part(1, columns.at[pl.ds(0, NY - 1), x], y_peer(1)).wait_recv()
        for d in range(1, NX):
            part(2, columns.at[:, x, c], x_peer(d)).start()

    def router_c():
        part(2, columns.at[:, pl.ds(0, NX - 1)], x_peer(1)).wait_recv()
        part(3, columns.at[:, :, c], c_peer).start()

    def router_out():
        part(3, columns, c_peer).wait_recv()
        for j in range(NZ * 2):
            piece = columns[:, :, :, j // 2, j % 2, :].reshape(NY * NX * NC, LANES)
            router_ref[:, j * LANES : (j + 1) * LANES] = piece.astype(jnp.bfloat16)

    stages = dict(zip(STAGES, (router_z, router_y, router_x)))
    for at, stage in zip(STAGES[3:], (router_c, router_out)):
        stages[at] = functools.partial(pl.when(jnp.logical_not(feeder)), stage)
    stages[MEET] = meet_across
    stages.update((at, functools.partial(meet_round, r)) for r, at in enumerate(MEET_ROUNDS))
    for step in range(STEPS):
        for k in range(CHUNKS):
            if step * CHUNKS + k < AHEAD:
                pl.when(jnp.logical_not(feeder))(functools.partial(forward, step, k))
            else:
                forward(step, k)
            for n in range(GROUP):
                if (step * CHUNKS + k) * GROUP + n in stages:
                    stages[(step * CHUNKS + k) * GROUP + n]()

    @pl.when(feeder)
    def _():
        router_c()
        router_out()

    sent = blocks_ref.at[pl.ds(0, 2 * STEPS)]
    remote(sent, send_sem, recv_sem.at[0], near[UP]).wait_send()
    for n in sorted({*SHARE[0], *SHARE[1], CORNER_SHARE}):
        if n > 0:
            up = blocks_ref.at[0, pl.ds(0, n)]
            pl.when(share_above == n)(remote(up, last_sem.at[UP], recv_last, near[UP]).wait_send)
        if n < PIECES:
            dn = blocks_ref.at[0, pl.ds(0, PIECES - n)]
            pl.when(share_below == n)(remote(dn, last_sem.at[DOWN], recv_last, near[DOWN]).wait_send)
    far = blocks_ref.at[lax.rem(z + NZ // 2, NZ)]
    remote(far, last_sem.at[UP], recv_last, near[UP]).wait_recv()


def place_kernel(blocks_ref, router_ref, down_out, router_out, sem, router_sem):
    for b in range(NZ):
        for k in range(PIECES):
            dst = down_out.at[pl.ds(b * CUT, CUT), pl.ds(k * LANES, LANES)]
            pltpu.make_async_copy(blocks_ref.at[b, k], dst, sem).start()
    router = pltpu.make_async_copy(router_ref, router_out, router_sem)
    router.start()
    pltpu.make_async_copy(blocks_ref, blocks_ref, sem).wait()
    router.wait()


def on_device(train_down, router_weight, router_gain):
    hbm = pl.BlockSpec(memory_space=pltpu.HBM)
    vmem = pl.BlockSpec(memory_space=pltpu.VMEM)
    owners = NY * NX * NC
    dma, plain = pltpu.SemaphoreType.DMA, pltpu.SemaphoreType.REGULAR
    blocks, router = pl.pallas_call(
        gather_kernel,
        name="gather",
        out_shape=(
            jax.ShapeDtypeStruct((NZ, PIECES, CUT, LANES), jnp.bfloat16),
            jax.ShapeDtypeStruct((owners, NZ * CUT), jnp.bfloat16),
        ),
        in_specs=[hbm] * 3,
        out_specs=(vmem, vmem),
        scratch_shapes=[
            pltpu.VMEM((EXPERT, CUT), jnp.float32),
            pltpu.VMEM((2, 2, LANES), jnp.float32),
            pltpu.VMEM((NZ, 2, LANES), jnp.bfloat16),
            pltpu.VMEM((NY, NX, NC, NZ, 2, LANES), jnp.float32),
            dma((2,)), dma, plain((NORTH + 1,)), plain((ROUNDS,)),
            dma, dma((2,)), dma((STEPS * CHUNKS,)), dma,
            dma((4,)),
        ],
        compiler_params=pltpu.CompilerParams(
            collective_id=0, has_side_effects=True, vmem_limit_bytes=16 << 20
        ),
    )(
        *(pltpu.with_memory_space_constraint(array, pltpu.HBM) for array in (
            train_down.reshape(EXPERT, CUT),
            router_weight.reshape(2, LANES),
            router_gain.reshape(2, LANES),
        )),
    )
    ready, serve = pl.pallas_call(
        place_kernel,
        name="place",
        out_shape=(
            jax.ShapeDtypeStruct((NZ * CUT, EXPERT), jnp.bfloat16),
            jax.ShapeDtypeStruct((owners, NZ * CUT), jnp.bfloat16),
        ),
        in_specs=[vmem, vmem],
        out_specs=(hbm, hbm),
        scratch_shapes=[dma, dma],
        compiler_params=pltpu.CompilerParams(vmem_limit_bytes=16 << 20),
    )(blocks, router)
    return ready[None], serve.T


def solution(mesh):
    in_specs = (P("owner", None, "rows"), P("rows", "owner"), P("rows"))
    out_specs = (P("owner", None, None), P())
    return jax.shard_map(
        on_device, mesh=mesh, in_specs=in_specs, out_specs=out_specs, check_vma=False
    )
```

```python
import functools

import jax
import jax.numpy as jnp
from jax import lax
from jax.experimental import pallas as pl
from jax.experimental.pallas import tpu as pltpu
from jax.sharding import PartitionSpec as P

MESH = pl.DeviceIdType.MESH
NY, NX, NC, NZ = 8, 4, 2, 8
EXPERT = 1024
CUT = 256
LANES = 128
PIECES = EXPERT // LANES
GROUP = 2
CHUNKS = PIECES // GROUP
STEPS = NZ // 2 - 1
ROUNDS = 3
SHARE = ((1, 4, 4, 4, 4, 4, 4, 6), (2, 4, 4, 4, 4, 4, 4, 6))
CORNER_SHARE = 1
STAGES = (8, 10, 15, 18, 20)
MEET, MEET_ROUNDS = 3, (5, 7, 9)
AHEAD = 2
UP, DOWN, NORTH, SOUTH, EAST, WEST, TWIN = range(7)
BACK = (DOWN, UP, SOUTH, NORTH, WEST, EAST, TWIN)


def share_of(corner, c, z):
    share = jnp.int32(0)
    for core in range(NC):
        for place in range(NZ):
            share = jnp.where(jnp.logical_and(c == core, z == place), jnp.int32(SHARE[core][place]), share)
    at_start = jnp.logical_and(corner, jnp.logical_and(c == NC - 1, z == 0))
    return jnp.where(at_start, jnp.int32(CORNER_SHARE), share)


def gather_kernel(
    down_ref, weight_ref, gain_ref,
    blocks_ref, router_ref,
    down, factors, rounded, columns,
    load_sem, small_sem, met_sem, across_sem,
    send_sem, last_sem, recv_sem, recv_last,
    part_sem,
):
    owner = lax.axis_index("owner")
    z = lax.axis_index("rows")
    c = lax.rem(owner, NC)
    x = lax.rem(owner // NC, NX)
    y = owner // (NC * NX)

    edges = (2, PIECES)
    loads = []
    for n, (low, high) in enumerate(zip((0, *edges), edges)):
        part = pl.ds(low * LANES, (high - low) * LANES)
        loads.append(pltpu.make_async_copy(down_ref.at[part], down.at[part], load_sem.at[n]))
    small = [
        pltpu.make_async_copy(weight_ref, factors.at[0], small_sem),
        pltpu.make_async_copy(gain_ref, factors.at[1], small_sem),
    ]
    loads[0].start()
    small[0].start()
    small[1].start()
    loads[1].start()

    def device(yy, xx, cc, zz):
        return {"owner": (yy * NX + xx) * NC + cc, "rows": zz}

    def z_peer(d):
        return device(y, x, c, lax.rem(z + d, NZ))

    def y_peer(d):
        return device(lax.rem(y + d, NY), x, c, z)

    def x_peer(d):
        return device(y, lax.rem(x + d, NX), c, z)

    c_peer = device(y, x, NC - 1 - c, z)
    near = [z_peer(1), z_peer(NZ - 1), y_peer(1), y_peer(NY - 1), x_peer(1), x_peer(NX - 1)]
    near.append(c_peer)
    later = [
        z != NZ - 1, z == 0,
        y < NY // 2, jnp.logical_or(y > NY // 2, y == 0),
        x != NX - 1, x == 0,
        c == NC - 1,
    ]
    place = ((c * NZ + z) * NY + y) * NX + x
    first = place == 0
    for i, at in ((DOWN, NY * NX), (NORTH, (NY - 1) * NX), (SOUTH, NX), (EAST, NX - 1), (WEST, 1)):
        later[i] = jnp.logical_or(later[i], place == at)
    for i in (UP, NORTH, SOUTH, EAST, WEST):
        later[i] = jnp.logical_and(later[i], jnp.logical_not(first))

    def tell(sem, peer):
        pl.semaphore_signal(sem, inc=1, device_id=peer, device_id_type=MESH)

    barrier = pltpu.get_barrier_semaphore()
    for peer, after in zip(near, later):
        pl.when(after)(functools.partial(tell, barrier, peer))
    earlier = sum(jnp.where(after, 0, 1) for after in later)

    def meet(i):
        pl.when(later[i])(lambda: pl.semaphore_wait(met_sem.at[i], 1))

    def met_at(i):
        return met_sem.at[min(BACK[i], NORTH)]

    corner = jnp.logical_and(y == 0, x == 0)
    share_above = share_of(corner, c, lax.rem(z + 1, NZ))
    share_below = share_of(corner, c, lax.rem(z + NZ - 1, NZ))

    def comes_up(share, n):
        few = share <= PIECES // 2
        return jnp.logical_or(jnp.logical_and(few, n < share), jnp.logical_and(jnp.logical_not(few), n >= PIECES - share))


    def turn(k):
        piece = down[k * LANES : (k + 1) * LANES, :]
        blocks_ref[z, k] = jnp.transpose(piece).astype(jnp.bfloat16)

    def remote(ref, send, recv, peer):
        return pltpu.make_async_remote_copy(
            src_ref=ref, dst_ref=ref, send_sem=send, recv_sem=recv,
            device_id=peer, device_id_type=MESH,
        )

    def chunk_of(block, k):
        return blocks_ref.at[lax.rem(block, NZ), pl.ds(k * GROUP, GROUP)]

    def copy_up(step, k, block):
        return remote(chunk_of(block, k), send_sem, recv_sem.at[step * CHUNKS + k], near[UP])

    def copy_dn(step, k, block):
        return remote(chunk_of(block, k), send_sem, recv_sem.at[step * CHUNKS + k], near[DOWN])

    def end_up(k):
        slot = blocks_ref.at[lax.rem(z + NZ - STEPS, NZ), k]
        return remote(slot, last_sem.at[UP], recv_last, near[UP])

    def end_dn(k):
        slot = blocks_ref.at[lax.rem(z + STEPS, NZ), k]
        return remote(slot, last_sem.at[DOWN], recv_last, near[DOWN])

    def own_up(n):
        remote(blocks_ref.at[z, n], send_sem, recv_sem.at[n // GROUP], near[UP]).start()

    def own_dn(n):
        remote(blocks_ref.at[z, n], send_sem, recv_sem.at[n // GROUP], near[DOWN]).start()

    pl.when(earlier > 0)(lambda: pl.semaphore_wait(barrier, earlier))
    for i, peer in enumerate(near):
        pl.when(jnp.logical_not(later[i]))(functools.partial(tell, met_at(i), peer))
    loads[0].wait()
    turn(0)
    turn(1)
    for n in range(PIECES):
        if n == 2:
            loads[1].wait()
            turn(2)
        if 2 <= n < PIECES - 1:
            turn(n + 1)
        pl.when(jnp.logical_not(later[DOWN]))(functools.partial(own_dn, n))
        pl.when(jnp.logical_not(later[UP]))(functools.partial(own_up, n))
    meet(UP)
    for n in range(PIECES):
        pl.when(later[UP])(functools.partial(own_up, n))
    pltpu.make_async_copy(factors, factors, small_sem).wait()
    rounded[z] = (factors[0] * factors[1]).astype(jnp.bfloat16)
    meet(DOWN)
    for n in range(PIECES):
        pl.when(later[DOWN])(functools.partial(own_dn, n))
    def forward(step, k):
        both = blocks_ref.at[0, pl.ds(0, 2 * GROUP)]
        remote(both, send_sem, recv_sem.at[step * CHUNKS + k], near[UP]).wait_recv()
        if step + 1 < STEPS:
            copy_up(step + 1, k, z + NZ - step - 1).start()
            copy_dn(step + 1, k, z + step + 1).start()
        else:
            for n in range(k * GROUP, (k + 1) * GROUP):
                pl.when(comes_up(share_above, n))(lambda n=n: end_up(n).start())
                pl.when(jnp.logical_not(comes_up(share_below, n)))(lambda n=n: end_dn(n).start())

    feeder = z == 1
    for k in range(AHEAD):
        pl.when(feeder)(functools.partial(forward, 0, k))
    for _ in range(ROUNDS):
        for i in (UP, DOWN):
            tell(met_at(i), near[i])
        for i in (UP, DOWN):
            pl.semaphore_wait(met_sem.at[i], 1)

    def meet_across():
        count = sum(jnp.where(after, 1, 0) for after in later[NORTH:])
        pl.when(count > 0)(lambda: pl.semaphore_wait(met_sem.at[NORTH], count))
        for peer in near[NORTH:TWIN]:
            tell(across_sem.at[0], peer)

    def meet_round(r):
        pl.semaphore_wait(across_sem.at[r], 4)
        if r + 1 < ROUNDS:
            for peer in near[NORTH:TWIN]:
                tell(across_sem.at[r + 1], peer)

    def part(i, ref, peer):
        return remote(ref, part_sem.at[i], part_sem.at[i], peer)

    own = rounded.at[z]
    for d in range(1, NZ):
        part(0, own, z_peer(d)).start()

    def router_z():
        part(0, columns.at[y, x, c, pl.ds(0, NZ - 1)], z_peer(1)).wait_recv()
        columns[y, x, c] = rounded[...].astype(jnp.float32)

    def router_y():
        for d in range(1, NY):
            part(1, columns.at[y, x, c], y_peer(d)).start()

    def router_x():
        part(1, columns.at[pl.ds(0, NY - 1), x], y_peer(1)).wait_recv()
        for d in range(1, NX):
            part(2, columns.at[:, x, c], x_peer(d)).start()

    def router_c():
        part(2, columns.at[:, pl.ds(0, NX - 1)], x_peer(1)).wait_recv()
        part(3, columns.at[:, :, c], c_peer).start()

    def router_out():
        part(3, columns, c_peer).wait_recv()
        for j in range(NZ * 2):
            piece = columns[:, :, :, j // 2, j % 2, :].reshape(NY * NX * NC, LANES)
            router_ref[:, j * LANES : (j + 1) * LANES] = piece.astype(jnp.bfloat16)

    stages = dict(zip(STAGES, (router_z, router_y, router_x)))
    for at, stage in zip(STAGES[3:], (router_c, router_out)):
        stages[at] = functools.partial(pl.when(jnp.logical_not(feeder)), stage)
    stages[MEET] = meet_across
    stages.update((at, functools.partial(meet_round, r)) for r, at in enumerate(MEET_ROUNDS))
    for step in range(STEPS):
        for k in range(CHUNKS):
            if step * CHUNKS + k < AHEAD:
                pl.when(jnp.logical_not(feeder))(functools.partial(forward, step, k))
            else:
                forward(step, k)
            for n in range(GROUP):
                if (step * CHUNKS + k) * GROUP + n in stages:
                    stages[(step * CHUNKS + k) * GROUP + n]()

    @pl.when(feeder)
    def _():
        router_c()
        router_out()

    sent = blocks_ref.at[pl.ds(0, 2 * STEPS)]
    remote(sent, send_sem, recv_sem.at[0], near[UP]).wait_send()
    for n in sorted({*SHARE[0], *SHARE[1], CORNER_SHARE}):
        if n > 0:
            up = blocks_ref.at[0, pl.ds(0, n)]
            pl.when(share_above == n)(remote(up, last_sem.at[UP], recv_last, near[UP]).wait_send)
        if n < PIECES:
            dn = blocks_ref.at[0, pl.ds(0, PIECES - n)]
            pl.when(share_below == n)(remote(dn, last_sem.at[DOWN], recv_last, near[DOWN]).wait_send)
    far = blocks_ref.at[lax.rem(z + NZ // 2, NZ)]
    remote(far, last_sem.at[UP], recv_last, near[UP]).wait_recv()


def place_kernel(blocks_ref, router_ref, down_out, router_out, sem, router_sem):
    for b in range(NZ):
        for k in range(PIECES):
            dst = down_out.at[pl.ds(b * CUT, CUT), pl.ds(k * LANES, LANES)]
            pltpu.make_async_copy(blocks_ref.at[b, k], dst, sem).start()
    router = pltpu.make_async_copy(router_ref, router_out, router_sem)
    router.start()
    pltpu.make_async_copy(blocks_ref, blocks_ref, sem).wait()
    router.wait()


def on_device(train_down, router_weight, router_gain):
    hbm = pl.BlockSpec(memory_space=pltpu.HBM)
    vmem = pl.BlockSpec(memory_space=pltpu.VMEM)
    owners = NY * NX * NC
    dma, plain = pltpu.SemaphoreType.DMA, pltpu.SemaphoreType.REGULAR
    blocks, router = pl.pallas_call(
        gather_kernel,
        name="gather",
        out_shape=(
            jax.ShapeDtypeStruct((NZ, PIECES, CUT, LANES), jnp.bfloat16),
            jax.ShapeDtypeStruct((owners, NZ * CUT), jnp.bfloat16),
        ),
        in_specs=[hbm] * 3,
        out_specs=(vmem, vmem),
        scratch_shapes=[
            pltpu.VMEM((EXPERT, CUT), jnp.float32),
            pltpu.VMEM((2, 2, LANES), jnp.float32),
            pltpu.VMEM((NZ, 2, LANES), jnp.bfloat16),
            pltpu.VMEM((NY, NX, NC, NZ, 2, LANES), jnp.float32),
            dma((2,)), dma, plain((NORTH + 1,)), plain((ROUNDS,)),
            dma, dma((2,)), dma((STEPS * CHUNKS,)), dma,
            dma((4,)),
        ],
        compiler_params=pltpu.CompilerParams(
            collective_id=0, has_side_effects=True, vmem_limit_bytes=16 << 20
        ),
    )(
        *(pltpu.with_memory_space_constraint(array, pltpu.HBM) for array in (
            train_down.reshape(EXPERT, CUT),
            router_weight.reshape(2, LANES),
            router_gain.reshape(2, LANES),
        )),
    )
    ready, serve = pl.pallas_call(
        place_kernel,
        name="place",
        out_shape=(
            jax.ShapeDtypeStruct((NZ * CUT, EXPERT), jnp.bfloat16),
            jax.ShapeDtypeStruct((owners, NZ * CUT), jnp.bfloat16),
        ),
        in_specs=[vmem, vmem],
        out_specs=(hbm, hbm),
        scratch_shapes=[dma, dma],
        compiler_params=pltpu.CompilerParams(vmem_limit_bytes=16 << 20),
    )(blocks, router)
    return ready[None], serve.T


def solution(mesh):
    in_specs = (P("owner", None, "rows"), P("rows", "owner"), P("rows"))
    out_specs = (P("owner", None, None), P())
    return jax.shard_map(
        on_device, mesh=mesh, in_specs=in_specs, out_specs=out_specs, check_vma=False
    )
```
